8 devices in a mesh: data: 8 (over z, y, x, core).
Axes of the slice: x: 2, y: 2, z: 1, core: 2. Of those that a mesh axis runs over, the one named last changes fastest.
Arguments:
- h_a: bfloat16 [8192, 2048], P('data')
- h_b: bfloat16 [8192, 2048], P('data')
- w_one: bfloat16 [2048, 1024], replicated
- w_two: bfloat16 [1024, 1024], replicated
- w_three: bfloat16 [1024, 1024], replicated
- gain_one: float32 [1024], replicated
- bias_one: float32 [1024], replicated
- gain_two: float32 [1024], replicated
- bias_two: float32 [1024], replicated
Outputs:
- output 1: float32 [], replicated
- output 2: float32 [2048, 1024], replicated
- output 3: float32 [1024, 1024], replicated
- output 4: float32 [1024, 1024], replicated
- output 5: float32 [1024], replicated
- output 6: float32 [1024], replicated
- output 7: float32 [1024], replicated
- output 8: float32 [1024], replicated
All inputs are finite; a program needn't handle non-finite values.
Results may differ from the reference program's by a relative error of at most 0.00107.
Values are sent between devices in bfloat16 or wider.
A program may use at most 1 GiB of HBM per device.

```python
import jax
import jax.numpy as jnp
from jax import lax

GROUP_DEVS = 8
ROWS_DEV = 1024
FEAT_DIM = 2048
PROJ_DIM = 1024

ALL_ROWS = GROUP_DEVS * ROWS_DEV
BN_EPS = 1e-5
STD_EPS = 1e-4
INV_WEIGHT = 2.0
VAR_WEIGHT = 1.0
COV_WEIGHT = 2.0


def setup_inputs(seed: int = 0) -> dict:
    key_list = jax.random.split(jax.random.key(seed), 11)
    shard_shape = (GROUP_DEVS, ROWS_DEV, FEAT_DIM)
    stat_shape = (GROUP_DEVS, 1, FEAT_DIM)
    base_a = jax.random.normal(key_list[0], shard_shape, jnp.float32)
    base_b = 0.8 * base_a + 0.6 * jax.random.normal(key_list[1], shard_shape, jnp.float32)
    shard_off = 0.6 * jax.random.normal(key_list[2], stat_shape, jnp.float32)
    shard_scale = jnp.exp(0.3 * jax.random.normal(key_list[3], stat_shape, jnp.float32))
    h_a = ((base_a + shard_off) * shard_scale).reshape(ALL_ROWS, FEAT_DIM).astype(jnp.bfloat16)
    h_b = ((base_b + shard_off) * shard_scale).reshape(ALL_ROWS, FEAT_DIM).astype(jnp.bfloat16)
    w_one = (jax.random.normal(key_list[4], (FEAT_DIM, PROJ_DIM), jnp.float32) * FEAT_DIM ** -0.5).astype(jnp.bfloat16)
    w_two = (jax.random.normal(key_list[5], (PROJ_DIM, PROJ_DIM), jnp.float32) * PROJ_DIM ** -0.5).astype(jnp.bfloat16)
    w_three = (jax.random.normal(key_list[6], (PROJ_DIM, PROJ_DIM), jnp.float32) * (0.7 * PROJ_DIM ** -0.5)).astype(jnp.bfloat16)
    gain_one = 1.0 + 0.3 * jax.random.normal(key_list[7], (PROJ_DIM,), jnp.float32)
    bias_one = 0.3 * jax.random.normal(key_list[8], (PROJ_DIM,), jnp.float32)
    gain_two = 1.0 + 0.3 * jax.random.normal(key_list[9], (PROJ_DIM,), jnp.float32)
    bias_two = 0.3 * jax.random.normal(key_list[10], (PROJ_DIM,), jnp.float32)
    return {'h_a': h_a, 'h_b': h_b, 'w_one': w_one, 'w_two': w_two, 'w_three': w_three,
            'gain_one': gain_one, 'bias_one': bias_one, 'gain_two': gain_two, 'bias_two': bias_two}


def layer_forward(x_in, weight, gain_vec, bias_vec):
    pre_act = jnp.dot(x_in, weight, preferred_element_type=jnp.float32)
    centered = pre_act - jnp.mean(pre_act, axis=0)
    inv_std = lax.rsqrt(jnp.mean(centered * centered, axis=0) + BN_EPS)
    normed = centered * inv_std
    act_val = gain_vec * normed + bias_vec
    return jnp.maximum(act_val, 0.0).astype(jnp.bfloat16), normed, act_val, inv_std


def layer_backward(d_out, normed, act_val, inv_std, gain_vec):
    d_act = jnp.where(act_val > 0.0, d_out, 0.0)
    sum_d = jnp.sum(d_act, axis=0)
    sum_dn = jnp.sum(d_act * normed, axis=0)
    d_pre = inv_std * gain_vec * (d_act - sum_d / ALL_ROWS - normed * (sum_dn / ALL_ROWS))
    return d_pre.astype(jnp.bfloat16), sum_dn, sum_d


def view_forward(view_feats, w_one, w_two, w_three, gain_one, bias_one, gain_two, bias_two):
    hidden_one, normed_one, act_one, inv_one = layer_forward(view_feats, w_one, gain_one, bias_one)
    hidden_two, normed_two, act_two, inv_two = layer_forward(hidden_one, w_two, gain_two, bias_two)
    z_view = jnp.dot(hidden_two, w_three, preferred_element_type=jnp.float32).astype(jnp.bfloat16)
    return z_view, (hidden_one, normed_one, act_one, inv_one, hidden_two, normed_two, act_two, inv_two)


def branch_terms(z_view):
    z_float = z_view.astype(jnp.float32)
    centered = z_float - jnp.mean(z_float, axis=0)
    cov_mat = jnp.dot(centered.T, centered) / (ALL_ROWS - 1)
    diag_var = jnp.diagonal(cov_mat)
    std_vec = jnp.sqrt(diag_var + STD_EPS)
    off_diag = cov_mat - jnp.diag(diag_var)
    hinge_on = (std_vec < 1.0).astype(jnp.float32)
    term_val = VAR_WEIGHT * jnp.sum(jnp.maximum(1.0 - std_vec, 0.0)) + COV_WEIGHT * jnp.sum(off_diag * off_diag)
    grad_cov = 2.0 * COV_WEIGHT * off_diag - jnp.diag(VAR_WEIGHT * hinge_on / (2.0 * std_vec))
    grad_hat = grad_cov.astype(jnp.bfloat16).astype(jnp.float32)
    grad_z = (2.0 / (ALL_ROWS - 1)) * jnp.dot(centered, grad_hat)
    return term_val, grad_z


def view_backward(view_feats, d_z, saved, w_two, w_three, gain_one, gain_two):
    hidden_one, normed_one, act_one, inv_one, hidden_two, normed_two, act_two, inv_two = saved
    grad_three = jnp.dot(hidden_two.T, d_z, preferred_element_type=jnp.float32)
    d_hidden_two = jnp.dot(d_z, w_three.T, preferred_element_type=jnp.float32)
    d_pre_two, gain_grad_two, bias_grad_two = layer_backward(d_hidden_two, normed_two, act_two, inv_two, gain_two)
    grad_two = jnp.dot(hidden_one.T, d_pre_two, preferred_element_type=jnp.float32)
    d_hidden_one = jnp.dot(d_pre_two, w_two.T, preferred_element_type=jnp.float32)
    d_pre_one, gain_grad_one, bias_grad_one = layer_backward(d_hidden_one, normed_one, act_one, inv_one, gain_one)
    grad_one = jnp.dot(view_feats.T, d_pre_one, preferred_element_type=jnp.float32)
    return grad_one, grad_two, grad_three, gain_grad_one, bias_grad_one, gain_grad_two, bias_grad_two


def reference(h_a, h_b, w_one, w_two, w_three, gain_one, bias_one, gain_two, bias_two):
    z_a, saved_a = view_forward(h_a, w_one, w_two, w_three, gain_one, bias_one, gain_two, bias_two)
    z_b, saved_b = view_forward(h_b, w_one, w_two, w_three, gain_one, bias_one, gain_two, bias_two)
    term_a, grad_za = branch_terms(z_a)
    term_b, grad_zb = branch_terms(z_b)
    z_diff = z_a.astype(jnp.float32) - z_b.astype(jnp.float32)
    loss_val = INV_WEIGHT * jnp.sum(z_diff * z_diff) / ALL_ROWS + term_a + term_b
    d_inv = (2.0 * INV_WEIGHT / ALL_ROWS) * z_diff
    d_za = (grad_za + d_inv).astype(jnp.bfloat16)
    d_zb = (grad_zb - d_inv).astype(jnp.bfloat16)
    back_a = view_backward(h_a, d_za, saved_a, w_two, w_three, gain_one, gain_two)
    back_b = view_backward(h_b, d_zb, saved_b, w_two, w_three, gain_one, gain_two)
    summed = [part_a + part_b for part_a, part_b in zip(back_a, back_b)]
    return (loss_val, summed[0], summed[1], summed[2], summed[3], summed[4], summed[5], summed[6])
```

```python
import functools

import jax
import jax.numpy as jnp
from jax import lax
from jax.experimental import pallas as pl
from jax.experimental.pallas import tpu as pltpu
from jax.sharding import PartitionSpec as P

BN_EPS = 1e-5
STD_EPS = 1e-4
F32 = jnp.float32
BF16 = jnp.bfloat16
MESH = pl.DeviceIdType.MESH
NDEV = 8
BLK = 256
PAIRS = [(0, 0), (1, 1), (2, 2), (3, 3), (0, 1), (0, 2), (0, 3), (1, 2), (1, 3), (2, 3)]


class Place:
    def __init__(self):
        me = lax.axis_index('data')
        self.me = me
        self.c = lax.rem(me, 2)
        self.x = lax.rem(me // 2, 2)
        self.y = me // 4

    def flip(self, dy, dx, dc):
        y = 1 - self.y if dy else self.y
        x = 1 - self.x if dx else self.x
        c = 1 - self.c if dc else self.c
        return y * 4 + x * 2 + c

    def peer(self, o):
        return self.flip(o & 4, o & 2, o & 1)


def entry_barrier(place):
    barrier = pltpu.get_barrier_semaphore()
    for o in range(1, NDEV):
        pl.semaphore_signal(barrier, inc=1, device_id=(place.peer(o),), device_id_type=MESH)
    pl.semaphore_wait(barrier, NDEV - 1)


class StatExchange:
    def __init__(self, place, src, rcv, ssem, rsem):
        self.place, self.src, self.rcv, self.ssem, self.rsem = place, src, rcv, ssem, rsem
        self.sent = []

    def copies(self, slot):
        place = self.place
        return [pltpu.make_async_remote_copy(
            src_ref=self.src.at[slot], dst_ref=self.rcv.at[slot, place.me],
            send_sem=self.ssem.at[slot, o], recv_sem=self.rsem.at[slot, o],
            device_id=(place.peer(o),), device_id_type=MESH) for o in range(1, NDEV)]

    def send(self, slot):
        self.rcv[slot, self.place.me] = self.src[slot]
        for cp in self.copies(slot):
            cp.start()
        self.sent.append(slot)

    def total(self, slot):
        for cp in self.copies(slot):
            cp.wait_recv()
        acc = self.rcv[slot, 0]
        for d in range(1, NDEV):
            acc = acc + self.rcv[slot, d]
        return acc

    def drain(self):
        for slot in self.sent:
            for cp in self.copies(slot):
                cp.wait_send()


class Reduce:
    def __init__(self, place, part, full, rc, r1, r2, ssem, rsem):
        self.place, self.part, self.full = place, part, full
        self.rc, self.r1, self.r2 = rc, r1, r2
        self.ssem, self.rsem = ssem, rsem
        self.rows = part.shape[0]
        place_pq = [(place.x, place.y), (place.y, place.x)]
        rows, c = self.rows, place.c
        al = rows // 16
        self.leaf_rows = al
        mo = lambda v: pl.multiple_of(v, al)
        self.half_mine = mo(c * (rows // 2))
        self.half_other = mo((1 - c) * (rows // 2))
        self.o1_mine, self.o1_other, self.o2_mine, self.o2_other = [], [], [], []
        for k, (p, q) in enumerate(place_pq):
            base = c * (rows // 2) + k * (rows // 4)
            self.o1_mine.append(mo(base + p * (rows // 8)))
            self.o1_other.append(mo(base + (1 - p) * (rows // 8)))
            self.o2_mine.append(mo(base + p * (rows // 8) + q * (rows // 16)))
            self.o2_other.append(mo(base + p * (rows // 8) + (1 - q) * (rows // 16)))
        self.dev_c = place.flip(0, 0, 1)
        self.dev_1 = [place.flip(0, 1, 0), place.flip(1, 0, 0)]
        self.dev_2 = [place.flip(1, 0, 0), place.flip(0, 1, 0)]

    def _cp(self, idx, src, dst, dev):
        return pltpu.make_async_remote_copy(src_ref=src, dst_ref=dst, send_sem=self.ssem.at[idx], recv_sem=self.rsem.at[idx],
                                            device_id=(dev,), device_id_type=MESH)

    def cp_c(self):
        return [self._cp(0, self.part.at[pl.ds(self.half_other, self.rows // 2)], self.rc, self.dev_c)]

    def cp_1(self):
        return [self._cp(1 + k, self.part.at[pl.ds(self.o1_other[k], self.rows // 8)], self.r1.at[k], self.dev_1[k]) for k in (0, 1)]

    def cp_2(self):
        return [self._cp(3 + k, self.part.at[pl.ds(self.o2_other[k], self.rows // 16)], self.r2.at[k], self.dev_2[k]) for k in (0, 1)]

    def cp_g2(self):
        return [self._cp(5 + k, self.full.at[pl.ds(self.o2_mine[k], self.rows // 16)],
                         self.full.at[pl.ds(self.o2_mine[k], self.rows // 16)], self.dev_2[k]) for k in (0, 1)]

    def cp_g1(self):
        return [self._cp(7 + k, self.full.at[pl.ds(self.o1_mine[k], self.rows // 8)],
                         self.full.at[pl.ds(self.o1_mine[k], self.rows // 8)], self.dev_1[k]) for k in (0, 1)]

    def cp_gc(self):
        half = pl.ds(self.half_mine, self.rows // 2)
        return [self._cp(9, self.full.at[half], self.full.at[half], self.dev_c)]

    @staticmethod
    def start(cps):
        for cp in cps:
            cp.start()

    def begin(self):
        self.start(self.cp_c())

    def step_1(self):
        self.cp_c()[0].wait_recv()
        mine = pl.ds(self.half_mine, self.rows // 2)
        self.part[mine] = self.part[mine] + self.rc[...]
        self.start(self.cp_1())

    def step_2(self):
        for k, cp in enumerate(self.cp_1()):
            cp.wait_recv()
            mine = pl.ds(self.o1_mine[k], self.rows // 8)
            self.part[mine] = self.part[mine] + self.r1[k]
            self.cp_2()[k].start()

    def step_3(self, finish):
        for k, cp in enumerate(self.cp_2()):
            cp.wait_recv()
            mine = pl.ds(self.o2_mine[k], self.rows // 16)
            self.full[mine] = finish(self.o2_mine[k], self.part[mine] + self.r2[k])
            self.cp_g2()[k].start()

    def step_4(self):
        for k, cp in enumerate(self.cp_g2()):
            cp.wait_recv()
            self.cp_g1()[k].start()

    def step_5(self):
        for cp in self.cp_g1():
            cp.wait_recv()
        self.start(self.cp_gc())

    def step_6(self):
        self.cp_gc()[0].wait_recv()

    def drain(self):
        for cp in self.cp_c() + self.cp_1() + self.cp_2() + self.cp_g2() + self.cp_g1() + self.cp_gc():
            cp.wait_send()


def matmul_stats(dst, lhs, rhs, n_cols, store_stats):
    def body(j, _):
        cols = pl.ds(pl.multiple_of(j * BLK, BLK), BLK)
        out = jnp.dot(lhs[...], rhs[:, cols], preferred_element_type=F32)
        dst[:, cols] = out
        store_stats(cols, out)
        return 0

    lax.fori_loop(0, n_cols // BLK, body, 0)


def fwd_kernel(all_rows, h_a, h_b, w1, w2, w3, affine,
               n1_o, x1_o, n2_o, x2_o, dz_o, inv_o, loss_o,
               hbuf, w1b, w2b, w3b, u1, x1, u2, x2, gram, ghat, mu_outer, rc, r1, r2,
               st_src, st_rcv, zs_src, zs_rcv, ls_src, ls_rcv,
               ld_sem, out_sem, st_ss, st_rs, zs_ss, zs_rs, ls_ss, ls_rs, rd_ss, rd_rs):
    dim = w2b.shape[0]
    rows = u1.shape[1]
    packed = gram.shape[1]
    place = Place()

    loads = {}

    def load(name, src, dst):
        cp = pltpu.make_async_copy(src, dst, ld_sem.at[len(loads)])
        loads[name] = cp
        cp.start()

    load('w1', w1, w1b)
    load('ha', h_a, hbuf.at[0])
    load('hb', h_b, hbuf.at[1])
    load('w2', w2, w2b)
    load('w3', w3, w3b)
    outs = []

    def put(src, dst):
        cp = pltpu.make_async_copy(src, dst, out_sem.at[len(outs)])
        outs.append(cp)
        cp.start()

    entry_barrier(place)

    stats = StatExchange(place, st_src, st_rcv, st_ss, st_rs)
    zstats = StatExchange(place, zs_src, zs_rcv, zs_ss, zs_rs)
    lstats = StatExchange(place, ls_src, ls_rcv, ls_ss, ls_rs)

    def store_moments(slot):
        def store(cols, out):
            st_src[slot, 0:1, cols] = jnp.sum(out, axis=0, keepdims=True)
            st_src[slot, 1:2, cols] = jnp.sum(out * out, axis=0, keepdims=True)
        return store

    def norm_relu(slot, v, layer, ubuf, xbuf):
        mom = stats.total(slot)
        mean = mom[0:1] / all_rows
        var = mom[1:2] / all_rows - mean * mean
        inv = lax.rsqrt(var + BN_EPS)
        inv_o[2 * layer + v:2 * layer + v + 1, :] = inv
        gain = affine[2 * layer:2 * layer + 1, :]
        bias = affine[2 * layer + 1:2 * layer + 2, :]

        def body(i, _):
            rws = pl.ds(pl.multiple_of(i * 64, 64), 64)
            n = (ubuf[v, rws, :] - mean) * inv
            ubuf[v, rws, :] = n
            xbuf[v, rws, :] = jnp.maximum(gain * n + bias, 0.0).astype(BF16)
            return 0

        lax.fori_loop(0, rows // 64, body, 0)

    zcol = pl.ds(dim, dim)
    dzcol = pl.ds(0, dim)

    loads['w1'].wait()
    loads['ha'].wait()
    matmul_stats(u1.at[0], hbuf.at[0], w1b, dim, store_moments(0))
    stats.send(0)
    loads['hb'].wait()
    matmul_stats(u1.at[1], hbuf.at[1], w1b, dim, store_moments(1))
    stats.send(1)
    loads['w2'].wait()
    loads['w3'].wait()
    norm_relu(0, 0, 0, u1, x1)
    put(u1.at[0], n1_o.at[0])
    put(x1.at[0], x1_o.at[0])
    matmul_stats(u2.at[0], x1.at[0], w2b, dim, store_moments(2))
    stats.send(2)
    norm_relu(1, 1, 0, u1, x1)
    put(u1.at[1], n1_o.at[1])
    put(x1.at[1], x1_o.at[1])
    matmul_stats(u2.at[1], x1.at[1], w2b, dim, store_moments(3))
    stats.send(3)

    def project(v):
        def body(j, _):
            cols = pl.ds(pl.multiple_of(j * BLK, BLK), BLK)
            zc = pl.ds(pl.multiple_of(dim + j * BLK, BLK), BLK)
            z = jnp.dot(x2[v], w3b[:, cols], preferred_element_type=F32).astype(BF16)
            hbuf[v, :, zc] = z
            zf = z.astype(F32)
            zs_src[0, v:v + 1, cols] = jnp.sum(zf, axis=0, keepdims=True)
            if v == 1:
                diff = hbuf[0, :, zc].astype(F32) - zf
                zs_src[0, 2:3, cols] = jnp.sum(diff * diff, axis=0, keepdims=True)
                zs_src[0, 3:4, cols] = jnp.zeros((1, BLK), F32)
            return 0

        lax.fori_loop(0, dim // BLK, body, 0)

    def gram_of(v):
        for b, (i, j) in enumerate(PAIRS):
            zi = hbuf[v, :, dim + i * BLK:dim + (i + 1) * BLK]
            zj = hbuf[v, :, dim + j * BLK:dim + (j + 1) * BLK]
            gram[v, b * BLK:(b + 1) * BLK, :] = lax.dot_general(zi, zj, (((0,), (0,)), ((), ())), preferred_element_type=F32)

    reds = [Reduce(place, gram.at[v], ghat.at[v], rc.at[v], r1.at[v], r2.at[v], rd_ss.at[v], rd_rs.at[v]) for v in (0, 1)]

    norm_relu(2, 0, 1, u2, x2)
    put(u2.at[0], n2_o.at[0])
    put(x2.at[0], x2_o.at[0])
    project(0)
    gram_of(0)
    reds[0].begin()
    norm_relu(3, 1, 1, u2, x2)
    put(u2.at[1], n2_o.at[1])
    put(x2.at[1], x2_o.at[1])
    project(1)
    zstats.send(0)
    reds[0].step_1()
    gram_of(1)
    reds[1].begin()

    ztot = zstats.total(0)
    mus = [ztot[v:v + 1] / all_rows for v in (0, 1)]
    sq_sum = jnp.sum(ztot[2:3])
    for v in (0, 1):
        for b, (i, j) in enumerate(PAIRS):
            col = jnp.transpose(jnp.broadcast_to(mus[v][:, i * BLK:(i + 1) * BLK], (BLK, BLK)))
            mu_outer[v, b * BLK:(b + 1) * BLK, :] = (all_rows * col) * mus[v][:, j * BLK:(j + 1) * BLK]
    ls_src[0] = jnp.zeros((1, 128), F32)

    def finish(v):
        def fin(row, acc):
            leaf = reds[v].leaf_rows
            prow = row + lax.broadcasted_iota(jnp.int32, (leaf, BLK), 0)
            col = lax.broadcasted_iota(jnp.int32, (leaf, BLK), 1)
            diag_block = prow < 4 * BLK
            eye = diag_block & (lax.rem(prow, BLK) == col)
            cov = (acc - mu_outer[v, pl.ds(row, leaf), :]) / (all_rows - 1)
            std = jnp.sqrt(cov + STD_EPS)
            hinge = jnp.where(eye, jnp.maximum(1.0 - std, 0.0), 0.0)
            off = jnp.where(eye, 0.0, cov * cov) * jnp.where(diag_block, 1.0, 2.0)
            term = jnp.sum(hinge + 2.0 * off, axis=0, keepdims=True)
            ls_src[0] = ls_src[0] + term[:, :128] + term[:, 128:]
            on = jnp.where(std < 1.0, 1.0, 0.0)
            return jnp.where(eye, -on / (2.0 * std), 4.0 * cov).astype(BF16)
        return fin

    def expand(v):
        for b, (i, j) in enumerate(PAIRS):
            blk = ghat[v, b * BLK:(b + 1) * BLK, :]
            w1b[v * dim + i * BLK:v * dim + (i + 1) * BLK, j * BLK:(j + 1) * BLK] = blk
            if i != j:
                w1b[v * dim + j * BLK:v * dim + (j + 1) * BLK, i * BLK:(i + 1) * BLK] = jnp.transpose(blk)

    def grad_z(v):
        mu = mus[v]
        hi = mu.astype(BF16)
        mid = (mu - hi.astype(F32)).astype(BF16)
        low = (mu - hi.astype(F32) - mid.astype(F32)).astype(BF16)
        parts = jnp.concatenate([hi, mid, low, jnp.zeros((13, dim), BF16)], axis=0)
        sign = 1.0 if v == 0 else -1.0

        def body(j, _):
            cols = pl.ds(pl.multiple_of(j * BLK, BLK), BLK)
            zc = pl.ds(pl.multiple_of(dim + j * BLK, BLK), BLK)
            g = w1b[v * dim:(v + 1) * dim, cols]
            mean_part = jnp.sum(jnp.dot(parts, g, preferred_element_type=F32), axis=0, keepdims=True)
            row_part = jnp.dot(hbuf[v, :, zcol], g, preferred_element_type=F32)
            diff = hbuf[0, :, zc].astype(F32) - hbuf[1, :, zc].astype(F32)
            dz = (2.0 / (all_rows - 1)) * (row_part - mean_part) + (sign * 4.0 / all_rows) * diff
            hbuf[v, :, cols] = dz.astype(BF16)
            return 0

        lax.fori_loop(0, dim // BLK, body, 0)
        put(hbuf.at[v, :, dzcol], dz_o.at[v])

    reds[1].step_1()
    reds[0].step_2()
    reds[1].step_2()
    reds[0].step_3(finish(0))
    reds[1].step_3(finish(1))
    lstats.send(0)
    reds[0].step_4()
    reds[0].step_5()
    reds[1].step_4()
    reds[0].step_6()
    expand(0)
    grad_z(0)
    reds[1].step_5()
    reds[1].step_6()
    expand(1)
    grad_z(1)
    loss_o[...] = jnp.broadcast_to(jnp.sum(lstats.total(0)) + 2.0 * sq_sum / all_rows, (8, 128))
    for ex in (stats, zstats, lstats):
        ex.drain()
    for red in reds:
        red.drain()
    for cp in outs:
        cp.wait()


def forward(n_dev, h_a, h_b, w1, w2, w3, affine):
    rows, feat = h_a.shape
    dim = w2.shape[0]
    all_rows = rows * n_dev
    packed = len(PAIRS) * BLK
    any_spec = pl.BlockSpec(memory_space=pl.ANY)
    vm = pl.BlockSpec(memory_space=pltpu.VMEM)
    wide = lambda dt: jax.ShapeDtypeStruct((2, rows, dim), dt)
    dma = pltpu.SemaphoreType.DMA
    return pl.pallas_call(
        functools.partial(fwd_kernel, all_rows),
        name='forward',
        out_shape=[wide(F32), wide(BF16), wide(F32), wide(BF16), wide(BF16),
                   jax.ShapeDtypeStruct((4, dim), F32), jax.ShapeDtypeStruct((8, 128), F32)],
        in_specs=[any_spec] * 5 + [vm],
        out_specs=[any_spec] * 5 + [vm, vm],
        scratch_shapes=[
            pltpu.VMEM((2, rows, feat), BF16), pltpu.VMEM((feat, dim), BF16), pltpu.VMEM((dim, dim), BF16), pltpu.VMEM((dim, dim), BF16),
            pltpu.VMEM((2, rows, dim), F32), pltpu.VMEM((2, rows, dim), BF16), pltpu.VMEM((2, rows, dim), F32), pltpu.VMEM((2, rows, dim), BF16),
            pltpu.VMEM((2, packed, BLK), F32), pltpu.VMEM((2, packed, BLK), BF16), pltpu.VMEM((2, packed, BLK), F32),
            pltpu.VMEM((2, packed // 2, BLK), F32), pltpu.VMEM((2, 2, packed // 8, BLK), F32), pltpu.VMEM((2, 2, packed // 16, BLK), F32),
            pltpu.VMEM((4, 2, dim), F32), pltpu.VMEM((4, NDEV, 2, dim), F32),
            pltpu.VMEM((1, 4, dim), F32), pltpu.VMEM((1, NDEV, 4, dim), F32),
            pltpu.VMEM((1, 1, 128), F32), pltpu.VMEM((1, NDEV, 1, 128), F32),
            dma((5,)), dma((10,)), dma((4, NDEV)), dma((4, NDEV)), dma((1, NDEV)), dma((1, NDEV)), dma((1, NDEV)), dma((1, NDEV)),
            dma((2, 10)), dma((2, 10))],
        compiler_params=pltpu.CompilerParams(collective_id=0, has_side_effects=True, vmem_limit_bytes=67043328),
    )(h_a, h_b, w1, w2, w3, affine)


def solution(mesh):
    n_dev = mesh.shape['data']

    def local_step(h_a, h_b, w_one, w_two, w_three, gain_one, bias_one, gain_two, bias_two):
        all_rows = h_a.shape[0] * n_dev
        affine = jnp.stack([gain_one, bias_one, gain_two, bias_two])
        norm1, x1, norm2, x2, d_z, inv, loss = forward(n_dev, h_a, h_b, w_one, w_two, w_three, affine)
        grad_three = jnp.einsum('vnk,vnd->kd', x2, d_z, preferred_element_type=F32)
        d_x2 = jnp.einsum('vnd,kd->vnk', d_z, w_three, preferred_element_type=F32)
        d_u2, d_gain_two, d_bias_two = layer_backward(d_x2, norm2, inv[2:4, None, :], gain_two, bias_two, all_rows)
        grad_two = jnp.einsum('vnk,vnd->kd', x1, d_u2, preferred_element_type=F32)
        d_x1 = jnp.einsum('vnd,kd->vnk', d_u2, w_two, preferred_element_type=F32)
        d_u1, d_gain_one, d_bias_one = layer_backward(d_x1, norm1, inv[0:2, None, :], gain_one, bias_one, all_rows)
        grad_one = (jnp.einsum('nf,nd->fd', h_a, d_u1[0], preferred_element_type=F32)
                    + jnp.einsum('nf,nd->fd', h_b, d_u1[1], preferred_element_type=F32))
        grad_one, grad_two, grad_three = lax.psum((grad_one, grad_two, grad_three), 'data')
        return loss[0, 0], grad_one, grad_two, grad_three, d_gain_one, d_bias_one, d_gain_two, d_bias_two

    row = P('data', None)
    return jax.shard_map(local_step, mesh=mesh, in_specs=(row, row) + (P(),) * 7, out_specs=(P(),) * 8, check_vma=False)


def layer_backward(d_out, normed, inv_std, gain_vec, bias_vec, all_rows):
    d_act = jnp.where(gain_vec * normed + bias_vec > 0.0, d_out, 0.0)
    sums = lax.psum(jnp.stack([jnp.sum(d_act, axis=1), jnp.sum(d_act * normed, axis=1)]), 'data')
    d_pre = inv_std * gain_vec * (d_act - sums[0][:, None, :] / all_rows - normed * (sums[1][:, None, :] / all_rows))
    return d_pre.astype(BF16), jnp.sum(sums[1], axis=0), jnp.sum(sums[0], axis=0)
```

```python
import functools

import jax
import jax.numpy as jnp
from jax import lax
from jax.experimental import pallas as pl
from jax.experimental.pallas import tpu as pltpu
from jax.sharding import PartitionSpec as P

BN_EPS = 1e-5
STD_EPS = 1e-4
F32 = jnp.float32
BF16 = jnp.bfloat16
MESH = pl.DeviceIdType.MESH
NDEV = 8
BLK = 256
STRIP = 64
SPARE = 524288
ROWS = 512
VMEM_BYTES = 67043328
LANES = 128
QUAD = 128
DIAG_ROWS = 4 * QUAD
TRI_ROWS = 6 * QUAD
OFF_PAIRS = [(0, 1), (0, 2), (0, 3), (1, 2), (1, 3), (2, 3)]
PIECES = []
for _i in range(4):
    _b = _i * BLK
    PIECES += [(_i * QUAD, 0, _b, _b, QUAD, False), (_i * QUAD, QUAD, _b, _b + QUAD, QUAD, True),
               (DIAG_ROWS + _i // 2 * QUAD, _i % 2 * QUAD, _b + QUAD, _b + QUAD, QUAD, False)]
PIECES += [(TRI_ROWS + _b * BLK, 0, _i * BLK, _j * BLK, BLK, True) for _b, (_i, _j) in enumerate(OFF_PAIRS)]
PACKED = TRI_ROWS + len(OFF_PAIRS) * BLK
SPLIT = TRI_ROWS + 2 * BLK
SPANS = ((0, SPLIT), (SPLIT, PACKED))
ROW0, ROW1 = slice(0, 1), slice(1, 2)
TN = (((0,), (0,)), ((), ()))
NT = (((1,), (1,)), ((), ()))


def dot(a, b, dims=(((1,), (0,)), ((), ()))):
    return lax.dot_general(a, b, dims, preferred_element_type=F32)


def col_sum(v):
    return jnp.sum(v, axis=0, keepdims=True)


def one(i):
    return slice(i, i + 1)


def tile(j, size=BLK, base=0):
    return pl.ds(pl.multiple_of(base + j * size, size), size)


def span(i, base=0):
    return slice(base + i * BLK, base + i * BLK + BLK)


def loop(count, body):
    def step(i, carry):
        body(i)
        return carry

    lax.fori_loop(0, count, step, 0)


class Place:
    def __init__(self):
        me = lax.axis_index('data')
        self.me = me
        self.c = lax.rem(me, 2)
        self.x = lax.rem(me // 2, 2)
        self.y = me // 4

    def flip(self, dy, dx, dc):
        y = 1 - self.y if dy else self.y
        x = 1 - self.x if dx else self.x
        c = 1 - self.c if dc else self.c
        return y * 4 + x * 2 + c

    def peer(self, o):
        return self.flip(o & 4, o & 2, o & 1)


def entry_barrier(place):
    barrier = pltpu.get_barrier_semaphore()
    for o in range(1, NDEV):
        pl.semaphore_signal(barrier, inc=1, device_id=(place.peer(o),), device_id_type=MESH)
    pl.semaphore_wait(barrier, NDEV - 1)


class StatExchange:
    def __init__(self, place, src, rcv, ssem, rsem):
        self.place, self.src, self.rcv, self.ssem, self.rsem = place, src, rcv, ssem, rsem
        self.sent = []

    def copies(self, slot):
        place = self.place
        return [pltpu.make_async_remote_copy(
            src_ref=self.src.at[slot], dst_ref=self.rcv.at[slot, place.me],
            send_sem=self.ssem.at[slot, o], recv_sem=self.rsem.at[slot, o],
            device_id=(place.peer(o),), device_id_type=MESH) for o in range(1, NDEV)]

    def send(self, slot):
        self.rcv[slot, self.place.me] = self.src[slot]
        for cp in self.copies(slot):
            cp.start()
        self.sent.append(slot)

    def total(self, slot):
        for cp in self.copies(slot):
            cp.wait_recv()
        acc = self.rcv[slot, 0]
        for d in range(1, NDEV):
            acc = acc + self.rcv[slot, d]
        return acc

    def drain(self):
        for slot in self.sent:
            for cp in self.copies(slot):
                cp.wait_send()


class Reduce:
    def __init__(self, place, part, full, rc, r1, r2, ssem, rsem):
        self.place, self.part, self.full = place, part, full
        self.ssem, self.rsem = ssem, rsem
        self.rows = part.shape[0]
        self.rc = rc.at[pl.ds(0, self.rows // 2)]
        self.r1 = [r1.at[k, pl.ds(0, self.rows // 8)] for k in (0, 1)]
        self.r2 = [r2.at[k, pl.ds(0, self.rows // 16)] for k in (0, 1)]
        place_pq = [(place.x, place.y), (place.y, place.x)]
        rows, c = self.rows, place.c
        al = rows // 16
        self.leaf_rows = al
        mo = lambda v: pl.multiple_of(v, al)
        self.half_mine = mo(c * (rows // 2))
        self.half_other = mo((1 - c) * (rows // 2))
        self.o1_mine, self.o1_other, self.o2_mine, self.o2_other = [], [], [], []
        for k, (p, q) in enumerate(place_pq):
            base = c * (rows // 2) + k * (rows // 4)
            self.o1_mine.append(mo(base + p * (rows // 8)))
            self.o1_other.append(mo(base + (1 - p) * (rows // 8)))
            self.o2_mine.append(mo(base + p * (rows // 8) + q * (rows // 16)))
            self.o2_other.append(mo(base + p * (rows // 8) + (1 - q) * (rows // 16)))
        self.dev_c = place.flip(0, 0, 1)
        self.dev_1 = [place.flip(0, 1, 0), place.flip(1, 0, 0)]
        self.dev_2 = [place.flip(1, 0, 0), place.flip(0, 1, 0)]

    def _cp(self, idx, src, dst, dev):
        return pltpu.make_async_remote_copy(src_ref=src, dst_ref=dst, send_sem=self.ssem.at[idx], recv_sem=self.rsem.at[idx],
                                            device_id=(dev,), device_id_type=MESH)

    def cp_c(self):
        return [self._cp(0, self.part.at[pl.ds(self.half_other, self.rows // 2)], self.rc, self.dev_c)]

    def cp_1(self):
        return [self._cp(1 + k, self.part.at[pl.ds(self.o1_other[k], self.rows // 8)], self.r1[k], self.dev_1[k]) for k in (0, 1)]

    def cp_2(self):
        return [self._cp(3 + k, self.part.at[pl.ds(self.o2_other[k], self.rows // 16)], self.r2[k], self.dev_2[k]) for k in (0, 1)]

    def cp_g2(self):
        return [self._cp(5 + k, self.full.at[pl.ds(self.o2_mine[k], self.rows // 16)],
                         self.full.at[pl.ds(self.o2_mine[k], self.rows // 16)], self.dev_2[k]) for k in (0, 1)]

    def cp_g1(self):
        return [self._cp(7 + k, self.full.at[pl.ds(self.o1_mine[k], self.rows // 8)],
                         self.full.at[pl.ds(self.o1_mine[k], self.rows // 8)], self.dev_1[k]) for k in (0, 1)]

    def cp_gc(self):
        half = pl.ds(self.half_mine, self.rows // 2)
        return [self._cp(9, self.full.at[half], self.full.at[half], self.dev_c)]

    @staticmethod
    def start(cps):
        for cp in cps:
            cp.start()

    def begin(self):
        self.start(self.cp_c())

    def step_1(self):
        self.cp_c()[0].wait_recv()
        mine = pl.ds(self.half_mine, self.rows // 2)
        self.part[mine] = self.part[mine] + self.rc[...]
        self.start(self.cp_1())

    def step_2(self):
        for k, (cp, nxt) in enumerate(zip(self.cp_1(), self.cp_2())):
            cp.wait_recv()
            mine = pl.ds(self.o1_mine[k], self.rows // 8)
            self.part[mine] = self.part[mine] + self.r1[k][...]
            nxt.start()

    def step_3(self, finish):
        for k, (cp, nxt) in enumerate(zip(self.cp_2(), self.cp_g2())):
            cp.wait_recv()
            mine = pl.ds(self.o2_mine[k], self.rows // 16)
            self.full[mine] = finish(self.o2_mine[k], self.part[mine] + self.r2[k][...])
            nxt.start()

    def step_4(self):
        for cp in self.cp_g2():
            cp.wait_recv()
        self.start(self.cp_g1())

    def step_5(self):
        for cp in self.cp_g1():
            cp.wait_recv()
        self.start(self.cp_gc())

    def step_6(self):
        self.cp_gc()[0].wait_recv()

    def drain(self):
        for cp in self.cp_c() + self.cp_1() + self.cp_2() + self.cp_g2() + self.cp_g1() + self.cp_gc():
            cp.wait_send()


GramReduce = Reduce


def by_rows(lhs, rhs, use, sums=0, dims=(((1,), (0,)), ((), ()))):
    def step(i, carry):
        rws = tile(i, ROWS)
        terms = use(rws, dot(lhs[rws, :], rhs[...], dims))
        return tuple(c + col_sum(t) for c, t in zip(carry, terms))

    width = rhs.shape[1 - dims[0][1][0]]
    return lax.fori_loop(0, lhs.shape[0] // ROWS, step, (jnp.zeros((1, width), F32),) * sums)


def fwd_kernel(all_rows, h_a, h_b, w1, w2, w3, g1, b1, g2, b2,
               n1_o, x1_o, n2_o, x2_o, dz_o, inv_o, loss_o,
               hbuf, w1b, w2b, w3b, u1, x1, u2, x2, gram, ghat, mu_outer, rc, r1, r2,
               st_src, st_rcv, zs_src, zs_rcv, ls_src, ls_rcv,
               ld_sem, out_sem, st_ss, st_rs, zs_ss, zs_rs, ls_ss, ls_rs, rd_ss, rd_rs):
    dim = w2b.shape[0]
    rows = u1.shape[1]
    affine = ((g1, b1), (g2, b2))
    place = Place()

    loads = {}

    def load(name, src, dst):
        cp = pltpu.make_async_copy(src, dst, ld_sem.at[len(loads)])
        loads[name] = cp
        cp.start()

    load('w1', w1, w1b)
    load('ha', h_a, hbuf.at[0])
    load('hb', h_b, hbuf.at[1])
    load('w2', w2, w2b)
    load('w3', w3, w3b)
    outs = []

    def put(src, dst):
        cp = pltpu.make_async_copy(src, dst, out_sem.at[len(outs)])
        outs.append(cp)
        cp.start()

    entry_barrier(place)

    stats = StatExchange(place, st_src, st_rcv, st_ss, st_rs)
    zstats = StatExchange(place, zs_src, zs_rcv, zs_ss, zs_rs)
    lstats = StatExchange(place, ls_src, ls_rcv, ls_ss, ls_rs)

    def linear(slot, dst, lhs, rhs):
        def use(rws, out):
            dst[rws, :] = out
            return out, out * out

        st_src[slot, ROW0, :], st_src[slot, ROW1, :] = by_rows(lhs, rhs, use, 2)
        stats.send(slot)

    def norm_relu(slot, v, layer, ubuf, xbuf):
        mom = stats.total(slot)
        mean = mom[ROW0] / all_rows
        var = mom[ROW1] / all_rows - mean * mean
        inv = lax.rsqrt(var + BN_EPS)
        inv_o[one(slot), :] = inv
        gain, bias = affine[layer]

        def body(i):
            rws = tile(i, STRIP)
            n = (ubuf[v, rws, :] - mean) * inv
            ubuf[v, rws, :] = n
            xbuf[v, rws, :] = jnp.maximum(gain[...] * n + bias[...], 0.0).astype(BF16)

        loop(rows // STRIP, body)

    zcol = pl.ds(dim, dim)
    dzcol = pl.ds(0, dim)
    zb = [hbuf.at[v, :, zcol] for v in (0, 1)]

    def project(v):
        def use(rws, out):
            z = out.astype(BF16)
            hbuf[v, rws, zcol] = z
            zf = z.astype(F32)
            if not v:
                return zf,
            diff = zb[0][rws, :].astype(F32) - zf
            return zf, diff * diff

        for o, term in enumerate(by_rows(x2.at[v], w3b, use, 1 + v)):
            zs_src[0, one(v + o), :] = term

    def gram_of(v, chunk):
        if not chunk:
            for i in range(dim // BLK):
                zi = hbuf[v, :, span(i, dim)]
                sq = dot(zi, zi, TN)
                for row, lane, r, c, size, _ in PIECES[3 * i:3 * i + 3]:
                    gram[v, row:row + size, lane:lane + size] = sq[r - i * BLK:r - i * BLK + size, c - i * BLK:c - i * BLK + size]
        lo, hi = SPANS[chunk]
        for b, (i, j) in enumerate(OFF_PAIRS):
            row = TRI_ROWS + b * BLK
            if lo <= row < hi:
                gram[v, row:row + BLK, :] = dot(hbuf[v, :, span(i, dim)], hbuf[v, :, span(j, dim)], TN)
        reds[v][chunk].begin()

    reds = []
    for v in (0, 1):
        pair = []
        for ch, (lo, hi) in enumerate(SPANS):
            rws = pl.ds(lo, hi - lo)
            pair.append(GramReduce(place, gram.at[v, rws], ghat.at[v, rws], rc.at[v, ch], r1.at[v, ch], r2.at[v, ch],
                                   rd_ss.at[v, ch], rd_rs.at[v, ch]))
        reds.append(pair)
    (a0, a1), (b0, b1) = reds

    def store_outer(mus):
        for v in (0, 1):
            for row, lane, r, c, size, _ in PIECES:
                col = jnp.transpose(jnp.broadcast_to(mus[v][:, r:r + size], (size, size)))
                mu_outer[v, row:row + size, lane:lane + size] = (all_rows * col) * mus[v][:, c:c + size]

    def finish(v, ch):
        def fin(row, acc):
            leaf = acc.shape[0]
            row = SPANS[ch][0] + row
            prow = row + lax.broadcasted_iota(jnp.int32, acc.shape, 0)
            lane = lax.broadcasted_iota(jnp.int32, acc.shape, 1)
            quad = (prow < TRI_ROWS) & ((prow >= DIAG_ROWS) | (lane < QUAD))
            eye = quad & (lax.rem(prow, QUAD) == lax.rem(lane, QUAD))
            cov = (acc - mu_outer[v, pl.ds(pl.multiple_of(row, 16), leaf), :]) / (all_rows - 1)
            std = jnp.sqrt(cov + STD_EPS)
            hinge = jnp.where(eye, jnp.maximum(1.0 - std, 0.0), 0.0)
            off = jnp.where(eye, 0.0, cov * cov) * jnp.where(quad, 1.0, 2.0)
            term = col_sum(hinge + 2.0 * off)
            ls_src[0] = ls_src[0] + term[:, :LANES] + term[:, LANES:]
            on = jnp.where(std < 1.0, 1.0, 0.0)
            return jnp.where(eye, -on / (2.0 * std), 4.0 * cov).astype(BF16)
        return fin

    def expand(v):
        for row, lane, r, c, size, mirrored in PIECES:
            blk = ghat[v, row:row + size, lane:lane + size]
            w1b[v * dim + r:v * dim + r + size, c:c + size] = blk
            if mirrored:
                w1b[v * dim + c:v * dim + c + size, r:r + size] = jnp.transpose(blk)

    def grad_z(v, mu, between):
        hi = mu.astype(BF16)
        mid = (mu - hi.astype(F32)).astype(BF16)
        low = (mu - hi.astype(F32) - mid.astype(F32)).astype(BF16)
        parts = jnp.concatenate([hi, mid, low, jnp.zeros((13, dim), BF16)], axis=0)
        g = w1b.at[pl.ds(v * dim, dim)]
        mean_part = col_sum(dot(parts, g[...]))
        sign = -1.0 if v else 1.0

        for part in range(rows // ROWS):
            sub = pl.ds(part * ROWS, ROWS)
            za, zo, out = zb[0].at[sub], zb[1].at[sub], hbuf.at[v, sub, dzcol]

            def use(rws, row_part):
                diff = za[rws, :].astype(F32) - zo[rws, :].astype(F32)
                dz = (2.0 / (all_rows - 1)) * (row_part - mean_part) + (sign * 4.0 / all_rows) * diff
                out[rws, :] = dz.astype(BF16)
                return ()

            by_rows(zb[v].at[sub], g, use)
            put(out, dz_o.at[v, sub])
            if between:
                between.pop(0)()

    loads['w1'].wait()
    loads['ha'].wait()
    linear(0, u1.at[0], hbuf.at[0], w1b)
    loads['hb'].wait()
    linear(1, u1.at[1], hbuf.at[1], w1b)
    loads['w2'].wait()
    loads['w3'].wait()
    for v in (0, 1):
        norm_relu(v, v, 0, u1, x1)
        put(u1.at[v], n1_o.at[v])
        put(x1.at[v], x1_o.at[v])
        linear(2 + v, u2.at[v], x1.at[v], w2b)
    zs_src[0] = jnp.zeros(zs_src.shape[1:], F32)
    ls_src[0] = jnp.zeros((1, LANES), F32)
    norm_relu(2, 0, 1, u2, x2)
    put(u2.at[0], n2_o.at[0])
    put(x2.at[0], x2_o.at[0])
    project(0)
    gram_of(0, 0)
    gram_of(0, 1)
    norm_relu(3, 1, 1, u2, x2)
    put(u2.at[1], n2_o.at[1])
    put(x2.at[1], x2_o.at[1])
    a0.step_1()
    a1.step_1()
    project(1)
    zstats.send(0)
    gram_of(1, 0)
    gram_of(1, 1)
    a0.step_2()
    ztot = zstats.total(0)
    mus = [ztot[one(v)] / all_rows for v in (0, 1)]
    sq_sum = jnp.sum(ztot[one(2)])
    b0.step_1()
    a1.step_2()
    b1.step_1()
    store_outer(mus)
    a0.step_3(finish(0, 0))
    a1.step_3(finish(0, 1))
    a0.step_4()
    b0.step_2()
    a1.step_4()
    b1.step_2()
    b0.step_3(finish(1, 0))
    a0.step_5()
    b1.step_3(finish(1, 1))
    lstats.send(0)
    a1.step_5()
    b0.step_4()
    b1.step_4()
    a0.step_6()
    a1.step_6()
    expand(0)
    grad_z(0, mus[0], [b0.step_5])
    b1.step_5()
    b0.step_6()
    b1.step_6()
    expand(1)
    grad_z(1, mus[1], [])
    loss_o[...] = jnp.broadcast_to(jnp.sum(lstats.total(0)) + 2.0 * sq_sum / all_rows, loss_o.shape)
    for ex in (stats, zstats, lstats):
        ex.drain()
    for red in (a0, a1, b0, b1):
        red.drain()
    for cp in outs:
        cp.wait()


def forward(n_dev, h_a, h_b, w1, w2, w3, *affine):
    rows, feat = h_a.shape
    dim = w2.shape[0]
    all_rows = rows * n_dev
    half = max(hi - lo for lo, hi in SPANS)
    any_spec = pl.BlockSpec(memory_space=pl.ANY)
    vm = pl.BlockSpec(memory_space=pltpu.VMEM)
    wide = lambda dt: jax.ShapeDtypeStruct((2, rows, dim), dt)
    dma = pltpu.SemaphoreType.DMA
    return pl.pallas_call(
        functools.partial(fwd_kernel, all_rows),
        name='forward',
        out_shape=[wide(F32), wide(BF16), wide(F32), wide(BF16), wide(BF16),
                   jax.ShapeDtypeStruct((4, dim), F32), jax.ShapeDtypeStruct((1, LANES), F32)],
        in_specs=[any_spec] * 5 + [vm] * 4,
        out_specs=[any_spec] * 5 + [vm, vm],
        scratch_shapes=[
            pltpu.VMEM((2, rows, feat), BF16), pltpu.VMEM((feat, dim), BF16), pltpu.VMEM((dim, dim), BF16), pltpu.VMEM((dim, dim), BF16),
            pltpu.VMEM((2, rows, dim), F32), pltpu.VMEM((2, rows, dim), BF16), pltpu.VMEM((2, rows, dim), F32), pltpu.VMEM((2, rows, dim), BF16),
            pltpu.VMEM((2, PACKED, BLK), F32), pltpu.VMEM((2, PACKED, BLK), BF16), pltpu.VMEM((2, PACKED, BLK), F32),
            pltpu.VMEM((2, 2, half // 2, BLK), F32), pltpu.VMEM((2, 2, 2, half // 8, BLK), F32), pltpu.VMEM((2, 2, 2, half // 16, BLK), F32),
            pltpu.VMEM((4, 2, dim), F32), pltpu.VMEM((4, NDEV, 2, dim), F32),
            pltpu.VMEM((1, 4, dim), F32), pltpu.VMEM((1, NDEV, 4, dim), F32),
            pltpu.VMEM((1, 1, LANES), F32), pltpu.VMEM((1, NDEV, 1, LANES), F32),
            dma((5,)), dma((12,)), dma((4, NDEV)), dma((4, NDEV)), dma((1, NDEV)), dma((1, NDEV)), dma((1, NDEV)), dma((1, NDEV)),
            dma((2, 2, 10)), dma((2, 2, 10))],
        compiler_params=pltpu.CompilerParams(collective_id=0, has_side_effects=True, vmem_limit_bytes=VMEM_BYTES),
    )(h_a, h_b, w1, w2, w3, *affine)


CHUNK = 256
PART_SLOTS = 4
LAST_STEP = 6


class Chunks:
    def __init__(self, place, count, part, rc, r1, r2, out, ssem, rsem):
        self.place, self.count = place, count
        self.part, self.rc, self.r1, self.r2, self.out = part, rc, r1, r2, out
        self.ssem, self.rsem = ssem, rsem

    def reduce(self, t):
        ps = lax.rem(t, PART_SLOTS)
        return Reduce(self.place, self.part.at[ps], self.out.at[tile(t, CHUNK)], self.rc.at[ps], self.r1.at[ps], self.r2.at[ps],
                      self.ssem.at[t], self.rsem.at[t])

    def step(self, k, t):
        red = self.reduce(t)
        if k == 3:
            red.step_3(lambda row, acc: acc)
            for cp in red.cp_c() + red.cp_1() + red.cp_2():
                cp.wait_send()
        else:
            getattr(red, 'step_%d' % k)()
        if k == LAST_STEP:
            for cp in red.cp_g2() + red.cp_g1() + red.cp_gc():
                cp.wait_send()

    def steps(self, t):
        for k in range(1, LAST_STEP + 1):
            if not isinstance(t, int) or 0 <= t - k < self.count:
                self.step(k, t - k)


def bwd_kernel(all_rows, dz, x2, n2, w3, x1, n1, w2, h_a, h_b, inv, g1, b1, g2, b2,
               out, bn_o,
               dzb, x2b, x1b, nb, dxb, dub, w2b, w3b, part, rc, r1, r2, st_src, st_rcv,
               ld_sem, n_sem, h_sem, st_ss, st_rs, rd_ss, rd_rs):
    dim = w2b.shape[0]
    rows = h_a.shape[0]
    feat = h_a.shape[1]
    affine = ((g1, b1), (g2, b2))
    place = Place()
    view = [slice(0, rows), slice(rows, 2 * rows)]
    lanes = lambda j: slice(j * CHUNK, (j + 1) * CHUNK)
    per = dim // CHUNK
    pairs = [('dz', dz, dzb)] + [('x2%d' % j, x2.at[:, lanes(j)], x2b.at[:, lanes(j)]) for j in range(per)]
    pairs += [('w3', w3, w3b)] + [('n2%d' % v, n2.at[view[v]], nb.at[view[v]]) for v in (0, 1)] + [('w2', w2, w2b), ('x1', x1, x1b)]
    loads = {}
    for i, (name, src, dst) in enumerate(pairs):
        loads[name] = pltpu.make_async_copy(src, dst, ld_sem.at[i])
        loads[name].start()
    load_n1 = [pltpu.make_async_copy(n1.at[view[v]], nb.at[view[v]], n_sem.at[v]) for v in (0, 1)]

    first_one = 2 * (dim // CHUNK)
    count = first_one + feat // CHUNK

    def load_h(t):
        slot = lax.rem(t, 2)
        cols = tile(t - first_one, CHUNK)
        return [pltpu.make_async_copy(h.at[:, cols], x2b.at[view[v], tile(slot, CHUNK)], h_sem.at[slot, v]) for v, h in enumerate((h_a, h_b))]

    entry_barrier(place)
    stats = StatExchange(place, st_src, st_rcv, st_ss, st_rs)
    chunks = Chunks(place, count, part, rc, r1, r2, out, rd_ss, rd_rs)

    def weight_grad(t, lhs, rhs):
        part[lax.rem(t, PART_SLOTS)] = dot(lhs, rhs, TN)
        chunks.reduce(t).begin()

    def grad_act(slot, v, layer, src, w):
        gain, bias = affine[layer]
        n_ref, dst = nb.at[view[v]], dxb.at[view[v]]

        def use(rws, dx):
            n = n_ref[rws, :]
            da = jnp.where(gain[...] * n + bias[...] > 0.0, dx, 0.0)
            dst[rws, :] = da
            return da, da * n

        st_src[slot, ROW0, :], st_src[slot, ROW1, :] = by_rows(src.at[view[v]], w, use, 2, NT)
        stats.send(slot)

    def grad_pre(slot, v, layer, dst):
        sums = stats.total(slot)
        for row, o in ((ROW1, 2 * layer), (ROW0, 2 * layer + 1)):
            bn_o[one(o), :] = bn_o[one(o), :] + sums[row] if v else sums[row]
        mean_d = sums[ROW0] / all_rows
        mean_dn = sums[ROW1] / all_rows
        scale = inv[one(2 * layer + v), :] * affine[layer][0][...]

        def body(i):
            rws = tile(i, STRIP, v * rows)
            dst[rws, :] = (scale * (dxb[rws, :] - mean_d - nb[rws, :] * mean_dn)).astype(BF16)

        loop(rows // STRIP, body)

    loads['dz'].wait()
    for t in range(first_one):
        chunks.steps(t)
        j = t % per
        if t == per:
            grad_pre(0, 0, 1, dub)
            load_n1[0].start()
            grad_pre(1, 1, 1, dub)
            load_n1[1].start()
            loads['x1'].wait()
            loads['w2'].wait()
        if t < per:
            loads['x2%d' % j].wait()
            weight_grad(t, x2b[:, lanes(j)], dzb[...])
        else:
            weight_grad(t, x1b[:, lanes(j)], dub[...])
        if t == per - 2:
            loads['w3'].wait()
            loads['n20'].wait()
            grad_act(0, 0, 1, dzb, w3b)
        if t == per - 1:
            loads['n21'].wait()
            grad_act(1, 1, 1, dzb, w3b)
        if t == per:
            load_n1[0].wait()
            grad_act(2, 0, 0, dub, w2b)
        if t == per + 1:
            load_n1[1].wait()
            grad_act(3, 1, 0, dub, w2b)
        if t == per + 2:
            grad_pre(2, 0, 0, dzb)
        if t == per + 3:
            grad_pre(3, 1, 0, dzb)
            for cp in load_h(first_one):
                cp.start()

    def tick(t, _):
        chunks.steps(t)
        for cp in load_h(t):
            cp.wait()

        @pl.when(t + 1 < count)
        def _():
            for cp in load_h(t + 1):
                cp.start()

        weight_grad(t, x2b[:, tile(lax.rem(t, 2), CHUNK)], dzb[...])
        return 0

    lax.fori_loop(first_one, count, tick, 0)
    for t in range(count, count + LAST_STEP):
        chunks.steps(t)
    stats.drain()


def backward(n_dev, dz, x2, n2, w3, x1, n1, w2, h_a, h_b, inv, *affine):
    rows, feat = h_a.shape
    dim = w2.shape[0]
    all_rows = rows * n_dev
    flat = lambda a: a.reshape(2 * rows, dim)
    any_spec = pl.BlockSpec(memory_space=pl.ANY)
    vm = pl.BlockSpec(memory_space=pltpu.VMEM)
    dma = pltpu.SemaphoreType.DMA
    count = (2 * dim + feat) // CHUNK
    big = (2 * rows, dim)
    grad_bytes = (2 * dim + feat) * dim * 4
    return pl.pallas_call(
        functools.partial(bwd_kernel, all_rows),
        name='backward',
        out_shape=[pltpu.VMEM((2 * dim + feat, dim), F32), pltpu.VMEM((4, dim), F32)],
        in_specs=[any_spec] * 9 + [vm] * 5,
        out_specs=[vm, vm],
        scratch_shapes=[
            pltpu.VMEM(big, BF16), pltpu.VMEM(big, BF16), pltpu.VMEM(big, BF16), pltpu.VMEM(big, F32), pltpu.VMEM(big, F32), pltpu.VMEM(big, BF16),
            pltpu.VMEM((dim, dim), BF16), pltpu.VMEM((dim, dim), BF16), pltpu.VMEM((PART_SLOTS, CHUNK, dim), F32),
            pltpu.VMEM((PART_SLOTS, CHUNK // 2, dim), F32), pltpu.VMEM((PART_SLOTS, 2, CHUNK // 8, dim), F32),
            pltpu.VMEM((PART_SLOTS, 2, CHUNK // 16, dim), F32),
            pltpu.VMEM((4, 2, dim), F32), pltpu.VMEM((4, NDEV, 2, dim), F32),
            dma((10,)), dma((2,)), dma((2, 2)), dma((4, NDEV)), dma((4, NDEV)), dma((count, 10)), dma((count, 10))],
        compiler_params=pltpu.CompilerParams(collective_id=1, has_side_effects=True, vmem_limit_bytes=VMEM_BYTES - grad_bytes - SPARE),
    )(flat(dz), flat(x2), flat(n2), w3, flat(x1), flat(n1), w2, h_a, h_b, inv, *affine)


def emit_kernel(rows, grads, bn, loss, *refs):
    big, small, (sem,) = refs[:3], refs[3:8], refs[8:]
    copies = [pltpu.make_async_copy(grads.at[pl.ds(lo, hi - lo)], dst, sem.at[i]) for i, (dst, (lo, hi)) in enumerate(zip(big, rows))]
    for cp in copies:
        cp.start()
    for i in range(4):
        small[i][...] = bn[one(i), :]
    small[4][...] = loss[...]
    for cp in copies:
        cp.wait()


def emit(grads, bn, loss, dim):
    total = grads.shape[0]
    rows = ((2 * dim, total), (dim, 2 * dim), (0, dim))
    any_spec = pl.BlockSpec(memory_space=pl.ANY)
    vm = pl.BlockSpec(memory_space=pltpu.VMEM)
    vec = jax.ShapeDtypeStruct((1, dim), F32)
    return pl.pallas_call(
        functools.partial(emit_kernel, rows),
        name='emit',
        out_shape=[jax.ShapeDtypeStruct((hi - lo, dim), F32) for lo, hi in rows] + [vec] * 4 + [jax.ShapeDtypeStruct((1, LANES), F32)],
        in_specs=[vm, vm, vm],
        out_specs=[any_spec] * 3 + [vm] * 5,
        scratch_shapes=[pltpu.SemaphoreType.DMA((3,))],
        compiler_params=pltpu.CompilerParams(vmem_limit_bytes=VMEM_BYTES // 16),
    )(pltpu.with_memory_space_constraint(grads, pltpu.VMEM), bn, loss)


def solution(mesh):
    n_dev = mesh.shape['data']

    def local_step(h_a, h_b, w_one, w_two, w_three, gain_one, bias_one, gain_two, bias_two):
        affine = [v.reshape(1, -1) for v in (gain_one, bias_one, gain_two, bias_two)]
        norm1, x1, norm2, x2, d_z, inv, loss = forward(n_dev, h_a, h_b, w_one, w_two, w_three, *affine)
        grads, bn = backward(n_dev, d_z, x2, norm2, w_three, x1, norm1, w_two, h_a, h_b, inv, *affine)
        d_one, d_two, d_three, *small, loss = emit(grads, bn, loss, w_two.shape[0])
        return (loss[0, 0], d_one, d_two, d_three) + tuple(v.reshape(-1) for v in small)

    row = P('data', None)
    return jax.shard_map(local_step, mesh=mesh, in_specs=(row, row) + (P(),) * 7, out_specs=(P(),) * 8, check_vma=False)
```

```python
import functools

import jax
import jax.numpy as jnp
from jax import lax
from jax.experimental import pallas as pl
from jax.experimental.pallas import tpu as pltpu
from jax.sharding import PartitionSpec as P

BN_EPS = 1e-5
STD_EPS = 1e-4
F32 = jnp.float32
BF16 = jnp.bfloat16
MESH = pl.DeviceIdType.MESH
NDEV = 8
BLK = 256
STRIP = 64
SPARE = 524288
ROWS = 512
VMEM_BYTES = 67043328
LANES = 128
QUAD = 128
DIAG_ROWS = 4 * QUAD
TRI_ROWS = 6 * QUAD
OFF_PAIRS = [(0, 1), (0, 2), (0, 3), (1, 2), (1, 3), (2, 3)]
PIECES = []
for _i in range(4):
    _b = _i * BLK
    PIECES += [(_i * QUAD, 0, _b, _b, QUAD, False), (_i * QUAD, QUAD, _b, _b + QUAD, QUAD, True),
               (DIAG_ROWS + _i // 2 * QUAD, _i % 2 * QUAD, _b + QUAD, _b + QUAD, QUAD, False)]
PIECES += [(TRI_ROWS + _b * BLK, 0, _i * BLK, _j * BLK, BLK, True) for _b, (_i, _j) in enumerate(OFF_PAIRS)]
PACKED = TRI_ROWS + len(OFF_PAIRS) * BLK
SPLIT = TRI_ROWS + 2 * BLK
SPANS = ((0, SPLIT), (SPLIT, PACKED))
ROW0, ROW1 = slice(0, 1), slice(1, 2)
TN = (((0,), (0,)), ((), ()))
NT = (((1,), (1,)), ((), ()))


def dot(a, b, dims=(((1,), (0,)), ((), ()))):
    return lax.dot_general(a, b, dims, preferred_element_type=F32)


def col_sum(v):
    return jnp.sum(v, axis=0, keepdims=True)


def one(i):
    return slice(i, i + 1)


def tile(j, size=BLK, base=0):
    return pl.ds(pl.multiple_of(base + j * size, size), size)


def span(i, base=0):
    return slice(base + i * BLK, base + i * BLK + BLK)


def loop(count, body):
    def step(i, carry):
        body(i)
        return carry

    lax.fori_loop(0, count, step, 0)


class Place:
    def __init__(self):
        me = lax.axis_index('data')
        self.me = me
        self.c = lax.rem(me, 2)
        self.x = lax.rem(me // 2, 2)
        self.y = me // 4

    def flip(self, dy, dx, dc):
        y = 1 - self.y if dy else self.y
        x = 1 - self.x if dx else self.x
        c = 1 - self.c if dc else self.c
        return y * 4 + x * 2 + c

    def peer(self, o):
        return self.flip(o & 4, o & 2, o & 1)


def entry_barrier(place):
    barrier = pltpu.get_barrier_semaphore()
    for o in range(1, NDEV):
        pl.semaphore_signal(barrier, inc=1, device_id=(place.peer(o),), device_id_type=MESH)
    pl.semaphore_wait(barrier, NDEV - 1)


class StatExchange:
    def __init__(self, place, src, rcv, ssem, rsem):
        self.place, self.src, self.rcv, self.ssem, self.rsem = place, src, rcv, ssem, rsem
        self.sent = []

    def copies(self, slot):
        place = self.place
        return [pltpu.make_async_remote_copy(
            src_ref=self.src.at[slot], dst_ref=self.rcv.at[slot, place.me],
            send_sem=self.ssem.at[slot, o], recv_sem=self.rsem.at[slot, o],
            device_id=(place.peer(o),), device_id_type=MESH) for o in range(1, NDEV)]

    def send(self, slot):
        self.rcv[slot, self.place.me] = self.src[slot]
        for cp in self.copies(slot):
            cp.start()
        self.sent.append(slot)

    def total(self, slot):
        for cp in self.copies(slot):
            cp.wait_recv()
        acc = self.rcv[slot, 0]
        for d in range(1, NDEV):
            acc = acc + self.rcv[slot, d]
        return acc

    def drain(self):
        for slot in self.sent:
            for cp in self.copies(slot):
                cp.wait_send()


class Reduce:
    def __init__(self, place, part, full, rc, r1, r2, ssem, rsem):
        self.place, self.part, self.full = place, part, full
        self.ssem, self.rsem = ssem, rsem
        self.rows = part.shape[0]
        self.rc, self.r1, self.r2 = rc, r1, r2
        place_pq = [(place.x, place.y), (place.y, place.x)]
        rows, c = self.rows, place.c
        al = rows // 16
        self.leaf_rows = al
        mo = lambda v: pl.multiple_of(v, al)
        self.half_mine = mo(c * (rows // 2))
        self.half_other = mo((1 - c) * (rows // 2))
        self.o1_mine, self.o1_other, self.o2_mine, self.o2_other = [], [], [], []
        for k, (p, q) in enumerate(place_pq):
            base = c * (rows // 2) + k * (rows // 4)
            self.o1_mine.append(mo(base + p * (rows // 8)))
            self.o1_other.append(mo(base + (1 - p) * (rows // 8)))
            self.o2_mine.append(mo(base + p * (rows // 8) + q * (rows // 16)))
            self.o2_other.append(mo(base + p * (rows // 8) + (1 - q) * (rows // 16)))
        self.dev_c = place.flip(0, 0, 1)
        self.dev_1 = [place.flip(0, 1, 0), place.flip(1, 0, 0)]
        self.dev_2 = [place.flip(1, 0, 0), place.flip(0, 1, 0)]

    def _cp(self, idx, src, dst, dev):
        return pltpu.make_async_remote_copy(src_ref=src, dst_ref=dst, send_sem=self.ssem.at[idx], recv_sem=self.rsem.at[idx],
                                            device_id=(dev,), device_id_type=MESH)

    def cp_c(self):
        return [self._cp(0, self.part.at[pl.ds(self.half_other, self.rows // 2)], self.rc, self.dev_c)]

    def cp_1(self):
        return [self._cp(1 + k, self.part.at[pl.ds(self.o1_other[k], self.rows // 8)], self.r1[k], self.dev_1[k]) for k in (0, 1)]

    def cp_2(self):
        return [self._cp(3 + k, self.part.at[pl.ds(self.o2_other[k], self.rows // 16)], self.r2[k], self.dev_2[k]) for k in (0, 1)]

    def cp_g2(self):
        return [self._cp(5 + k, self.full.at[pl.ds(self.o2_mine[k], self.rows // 16)],
                         self.full.at[pl.ds(self.o2_mine[k], self.rows // 16)], self.dev_2[k]) for k in (0, 1)]

    def cp_g1(self):
        return [self._cp(7 + k, self.full.at[pl.ds(self.o1_mine[k], self.rows // 8)],
                         self.full.at[pl.ds(self.o1_mine[k], self.rows // 8)], self.dev_1[k]) for k in (0, 1)]

    def cp_gc(self):
        half = pl.ds(self.half_mine, self.rows // 2)
        return [self._cp(9, self.full.at[half], self.full.at[half], self.dev_c)]

    @staticmethod
    def start(cps):
        for cp in cps:
            cp.start()

    def begin(self):
        self.start(self.cp_c())

    def step_1(self):
        self.cp_c()[0].wait_recv()
        mine = pl.ds(self.half_mine, self.rows // 2)
        self.part[mine] = self.part[mine] + self.rc[...]
        self.start(self.cp_1())

    def step_2(self):
        for k, (cp, nxt) in enumerate(zip(self.cp_1(), self.cp_2())):
            cp.wait_recv()
            mine = pl.ds(self.o1_mine[k], self.rows // 8)
            self.part[mine] = self.part[mine] + self.r1[k][...]
            nxt.start()

    def step_3(self, finish):
        for k, (cp, nxt) in enumerate(zip(self.cp_2(), self.cp_g2())):
            cp.wait_recv()
            mine = pl.ds(self.o2_mine[k], self.rows // 16)
            self.full[mine] = finish(self.o2_mine[k], self.part[mine] + self.r2[k][...])
            nxt.start()

    def step_4(self):
        for cp in self.cp_g2():
            cp.wait_recv()
        self.start(self.cp_g1())

    def step_5(self):
        for cp in self.cp_g1():
            cp.wait_recv()
        self.start(self.cp_gc())

    def step_6(self):
        self.cp_gc()[0].wait_recv()

    def drain_part(self):
        for cp in self.cp_c() + self.cp_1() + self.cp_2():
            cp.wait_send()

    def drain_full(self):
        for cp in self.cp_g2() + self.cp_g1() + self.cp_gc():
            cp.wait_send()


def by_rows(lhs, rhs, use, sums=0, dims=(((1,), (0,)), ((), ()))):
    def step(i, carry):
        rws = tile(i, ROWS)
        terms = use(rws, dot(lhs[rws, :], rhs[...], dims))
        return tuple(c + col_sum(t) for c, t in zip(carry, terms))

    width = rhs.shape[1 - dims[0][1][0]]
    return lax.fori_loop(0, lhs.shape[0] // ROWS, step, (jnp.zeros((1, width), F32),) * sums)


CHUNK, SMALL = 256, 128
LEAD, EVEN, TAIL = 0, 16, 0
COUNT = LEAD + EVEN + TAIL
PART_SLOTS, CORE_SLOTS, LINK_SLOTS = 3, 2, 4
LAST_STEP = 6


def chunk_of(t):
    if not isinstance(t, int) or LEAD <= t < LEAD + EVEN:
        return (t - LEAD) * CHUNK + LEAD * SMALL, CHUNK
    if t < LEAD:
        return t * SMALL, SMALL
    return EVEN * CHUNK + (t - EVEN) * SMALL, SMALL


class Chunks:
    def __init__(self, place, part, net, out, ssem, rsem):
        self.place, self.part, self.net, self.out = place, part, net, out
        self.ssem, self.rsem = ssem, rsem

    def reduce(self, t):
        row, size = chunk_of(t)
        link = lax.rem(t, LINK_SLOTS)

        def landing(base, slot, room, used):
            return self.net.at[pl.ds(pl.multiple_of(base + slot * room, 8), used)]

        one_base = CORE_SLOTS * CHUNK // 2
        two_base = one_base + LINK_SLOTS * CHUNK // 4
        return Reduce(self.place, self.part_of(t), self.out.at[pl.ds(pl.multiple_of(row, SMALL), size)],
                      landing(0, lax.rem(t, CORE_SLOTS), CHUNK // 2, size // 2),
                      [landing(one_base, 2 * link + k, CHUNK // 8, size // 8) for k in (0, 1)],
                      [landing(two_base, 2 * link + k, CHUNK // 16, size // 16) for k in (0, 1)], self.ssem.at[t], self.rsem.at[t])

    def part_of(self, t):
        return self.part.at[pl.ds(pl.multiple_of(lax.rem(t, PART_SLOTS) * CHUNK, CHUNK), chunk_of(t)[1])]

    def step(self, k, t):
        red = self.reduce(t)
        if k == 3:
            red.step_3(lambda row, acc: acc)
            red.drain_part()
        else:
            getattr(red, 'step_%d' % k)()
        if k == LAST_STEP:
            red.drain_full()

    def steps(self, t):
        for k in range(1, LAST_STEP + 1):
            if not isinstance(t, int) or 0 <= t - k < COUNT:
                self.step(k, t - k)


GramReduce = Reduce


def step_kernel(all_rows, h_a, h_b, w1, w2, w3, g1, b1, g2, b2,
                grads, bn_o, loss_o, n1_o,
                hbuf, w1b, w2b, w3b, x1, x2, nb, ghat, part, net, invs,
                st_src, st_rcv, zs_src, zs_rcv, ls_src, ls_rcv,
                ld_sem, n_sem, h_sem, st_ss, st_rs, zs_ss, zs_rs, ls_ss, ls_rs, gr_ss, gr_rs, rd_ss, rd_rs):
    dim = w2b.shape[0]
    rows, feat = h_a.shape
    affine = ((g1, b1), (g2, b2))
    view = [slice(0, rows), slice(rows, 2 * rows)]
    low, high = slice(0, 2 * dim), slice(2 * dim, 2 * dim + feat)
    u1, dxb = grads.at[low], grads.at[high]
    place = Place()
    h_all = (h_a, h_b)
    loads = {}
    for name, src, dst in (('w1', w1, w1b), ('ha', h_a, hbuf.at[view[0]]), ('hb', h_b, hbuf.at[view[1]]), ('w2', w2, w2b), ('w3', w3, w3b)):
        loads[name] = pltpu.make_async_copy(src, dst, ld_sem.at[len(loads)])
        loads[name].start()
    spill = [pltpu.make_async_copy(u1.at[view[v]], n1_o.at[view[v]], n_sem.at[v]) for v in (0, 1)]
    load_n1 = [pltpu.make_async_copy(n1_o.at[view[v]], nb.at[view[v]], n_sem.at[v]) for v in (0, 1)]

    def lanes(row, size):
        return pl.ds(pl.multiple_of(row, SMALL), size)

    entry_barrier(place)
    stats = StatExchange(place, st_src, st_rcv, st_ss, st_rs)
    zstats = StatExchange(place, zs_src, zs_rcv, zs_ss, zs_rs)
    lstats = StatExchange(place, ls_src, ls_rcv, ls_ss, ls_rs)

    def linear(slot, dst, lhs, rhs):
        def use(rws, out):
            dst[rws, :] = out
            return out, out * out

        st_src[slot, ROW0, :], st_src[slot, ROW1, :] = by_rows(lhs, rhs, use, 2)
        stats.send(slot)

    def norm_relu(slot, v, layer, ubuf, xbuf):
        mom = stats.total(slot)
        mean = mom[ROW0] / all_rows
        var = mom[ROW1] / all_rows - mean * mean
        inv = lax.rsqrt(var + BN_EPS)
        invs[one(slot), :] = inv
        gain, bias = affine[layer]

        def body(i):
            rws = tile(i, STRIP, v * rows)
            n = (ubuf[rws, :] - mean) * inv
            ubuf[rws, :] = n
            xbuf[rws, :] = jnp.maximum(gain[...] * n + bias[...], 0.0).astype(BF16)

        loop(rows // STRIP, body)

    zcol = pl.ds(dim, dim)
    dzb = hbuf.at[:, pl.ds(0, dim)]
    zb = [hbuf.at[view[v], zcol] for v in (0, 1)]

    def project(v):
        def use(rws, out):
            z = out.astype(BF16)
            zb[v][rws, :] = z
            zf = z.astype(F32)
            if not v:
                return zf,
            diff = zb[0][rws, :].astype(F32) - zf
            return zf, diff * diff

        for o, term in enumerate(by_rows(x2.at[view[v]], w3b, use, 1 + v)):
            zs_src[0, one(v + o), :] = term

    outer, gram = grads.at[low], grads.at[high]

    def band(v, ch):
        return pl.ds((2 * v + ch) * BLK, BLK)

    def packed_at(ref, v, row, lane, size):
        ch = int(row >= SPLIT)
        return ref.at[pl.ds(row - SPANS[ch][0], size), pl.ds((2 * v + ch) * BLK + lane, size)]

    gram_at = functools.partial(packed_at, gram)

    def gram_of(v, chunk):
        if not chunk:
            for i in range(dim // BLK):
                zi = hbuf[view[v], span(i, dim)]
                sq = dot(zi, zi, TN)
                for row, lane, r, c, size, _ in PIECES[3 * i:3 * i + 3]:
                    gram_at(v, row, lane, size)[...] = sq[r - i * BLK:r - i * BLK + size, c - i * BLK:c - i * BLK + size]
        lo, hi = SPANS[chunk]
        for b, (i, j) in enumerate(OFF_PAIRS):
            row = TRI_ROWS + b * BLK
            if lo <= row < hi:
                gram_at(v, row, 0, BLK)[...] = dot(hbuf[view[v], span(i, dim)], hbuf[view[v], span(j, dim)], TN)
        reds[v][chunk].begin()

    reds = []
    for v in (0, 1):
        pair = []
        for ch, (lo, hi) in enumerate(SPANS):
            n, bd = hi - lo, band(v, ch)
            r1 = [net.at[pl.ds(k * n // 8, n // 8), bd] for k in (0, 1)]
            r2 = [net.at[pl.ds(n // 4 + k * n // 16, n // 16), bd] for k in (0, 1)]
            pair.append(GramReduce(place, gram.at[pl.ds(0, n), bd], ghat.at[v, pl.ds(lo, n)], part.at[pl.ds(0, n // 2), bd], r1, r2,
                                   gr_ss.at[v, ch], gr_rs.at[v, ch]))
        reds.append(pair)
    (a0, a1), (b0, b1) = reds

    def store_outer(mus):
        for v in (0, 1):
            for row, lane, r, c, size, _ in PIECES:
                col = jnp.transpose(jnp.broadcast_to(mus[v][:, r:r + size], (size, size)))
                packed_at(outer, v, row, lane, size)[...] = (all_rows * col) * mus[v][:, c:c + size]

    def finish(v, ch):
        def fin(row, acc):
            leaf = acc.shape[0]
            prow = SPANS[ch][0] + row + lax.broadcasted_iota(jnp.int32, acc.shape, 0)
            lane = lax.broadcasted_iota(jnp.int32, acc.shape, 1)
            quad = (prow < TRI_ROWS) & ((prow >= DIAG_ROWS) | (lane < QUAD))
            eye = quad & (lax.rem(prow, QUAD) == lax.rem(lane, QUAD))
            cov = (acc - outer[pl.ds(row, leaf), band(v, ch)]) / (all_rows - 1)
            std = jnp.sqrt(cov + STD_EPS)
            hinge = jnp.where(eye, jnp.maximum(1.0 - std, 0.0), 0.0)
            off = jnp.where(eye, 0.0, cov * cov) * jnp.where(quad, 1.0, 2.0)
            term = col_sum(hinge + 2.0 * off)
            ls_src[0] = ls_src[0] + term[:, :LANES] + term[:, LANES:]
            on = jnp.where(std < 1.0, 1.0, 0.0)
            return jnp.where(eye, -on / (2.0 * std), 4.0 * cov).astype(BF16)
        return fin

    def expand(v):
        for row, lane, r, c, size, mirrored in PIECES:
            blk = ghat[v, row:row + size, lane:lane + size]
            w1b[v * dim + r:v * dim + r + size, c:c + size] = blk
            if mirrored:
                w1b[v * dim + c:v * dim + c + size, r:r + size] = jnp.transpose(blk)

    def grad_z(v, mu, between):
        hi = mu.astype(BF16)
        mid = (mu - hi.astype(F32)).astype(BF16)
        low = (mu - hi.astype(F32) - mid.astype(F32)).astype(BF16)
        parts = jnp.concatenate([hi, mid, low, jnp.zeros((13, dim), BF16)], axis=0)
        g = w1b.at[pl.ds(v * dim, dim)]
        mean_part = col_sum(dot(parts, g[...]))
        sign = -1.0 if v else 1.0

        for part in range(rows // ROWS):
            sub = pl.ds(part * ROWS, ROWS)
            za, zo, out = zb[0].at[sub], zb[1].at[sub], dzb.at[pl.ds(v * rows + part * ROWS, ROWS)]

            def use(rws, row_part):
                diff = za[rws, :].astype(F32) - zo[rws, :].astype(F32)
                dz = (2.0 / (all_rows - 1)) * (row_part - mean_part) + (sign * 4.0 / all_rows) * diff
                out[rws, :] = dz.astype(BF16)
                return ()

            by_rows(zb[v].at[sub], g, use)
            if between:
                between.pop(0)()

    chunks = Chunks(place, part, net, grads, rd_ss, rd_rs)

    def load_h(t):
        row, size = chunk_of(t)
        slot = lax.rem(t, 2)
        return [pltpu.make_async_copy(h.at[:, lanes(row - 2 * dim, size)], x2.at[view[v], lanes(slot * CHUNK, size)], h_sem.at[slot, v])
                for v, h in enumerate(h_all)]

    def weight_grad(t, lhs, rhs):
        dst = chunks.part_of(t)

        def half(j):
            cols = tile(j, ROWS)
            dst[:, cols] = dot(lhs[...], rhs[:, cols], TN)

        loop(dim // ROWS, half)
        chunks.reduce(t).begin()

    def grad_act(slot, v, layer, src, w):
        gain, bias = affine[layer]
        n_ref, dst = nb.at[view[v]], dxb.at[view[v]]

        def use(rws, dx):
            n = n_ref[rws, :]
            da = jnp.where(gain[...] * n + bias[...] > 0.0, dx, 0.0)
            dst[rws, :] = da
            return da, da * n

        st_src[slot, ROW0, :], st_src[slot, ROW1, :] = by_rows(src.at[view[v]], w, use, 2, NT)
        stats.send(slot)

    def grad_pre(slot, v, layer, dst):
        sums = stats.total(slot)
        for row, o in ((ROW1, 2 * layer), (ROW0, 2 * layer + 1)):
            bn_o[one(o), :] = bn_o[one(o), :] + sums[row] if v else sums[row]
        mean_d = sums[ROW0] / all_rows
        mean_dn = sums[ROW1] / all_rows
        scale = invs[one(2 * layer + v), :] * affine[layer][0][...]

        def body(i):
            rws = tile(i, STRIP, v * rows)
            dst[rws, :] = (scale * (dxb[rws, :] - mean_d - nb[rws, :] * mean_dn)).astype(BF16)

        loop(rows // STRIP, body)

    loads['w1'].wait()
    loads['ha'].wait()
    linear(0, u1.at[view[0]], hbuf.at[view[0]], w1b)
    loads['hb'].wait()
    linear(1, u1.at[view[1]], hbuf.at[view[1]], w1b)
    loads['w2'].wait()
    loads['w3'].wait()
    for v in (0, 1):
        norm_relu(v, v, 0, u1, x1)
        spill[v].start()
        linear(2 + v, nb.at[view[v]], x1.at[view[v]], w2b)
    zs_src[0] = jnp.zeros(zs_src.shape[1:], F32)
    ls_src[0] = jnp.zeros((1, LANES), F32)
    norm_relu(2, 0, 1, nb, x2)
    project(0)
    gram_of(0, 0)
    gram_of(0, 1)
    norm_relu(3, 1, 1, nb, x2)
    a0.step_1()
    a1.step_1()
    project(1)
    zstats.send(0)
    gram_of(1, 0)
    gram_of(1, 1)
    a0.step_2()
    ztot = zstats.total(0)
    mus = [ztot[one(v)] / all_rows for v in (0, 1)]
    sq_sum = jnp.sum(ztot[one(2)])
    b0.step_1()
    a1.step_2()
    b1.step_1()
    for cp in spill:
        cp.wait()
    store_outer(mus)
    a0.step_3(finish(0, 0))
    a1.step_3(finish(0, 1))
    a0.step_4()
    b0.step_2()
    a1.step_4()
    b1.step_2()
    b0.step_3(finish(1, 0))
    a0.step_5()
    b1.step_3(finish(1, 1))
    lstats.send(0)
    a1.step_5()
    b0.step_4()
    b1.step_4()
    a0.step_6()
    a1.step_6()
    expand(0)
    grad_z(0, mus[0], [b0.step_5])
    lead = lanes(0, chunk_of(0)[1])
    chunks.part_of(0)[...] = dot(x2[view[0], lead], dzb[view[0], :], TN)
    b1.step_5()
    b0.step_6()
    b1.step_6()
    expand(1)
    grad_z(1, mus[1], [])
    for red in (a0, a1, b0, b1):
        red.drain_part()

    dub, du1 = w1b, hbuf.at[:, zcol]
    first_two = next(t for t in range(COUNT) if chunk_of(t)[0] >= dim)
    first_one = next(t for t in range(COUNT) if chunk_of(t)[0] >= 2 * dim)
    extra = {
        first_two - 2: lambda: grad_act(4, 0, 1, dzb, w3b),
        first_two - 1: lambda: grad_act(5, 1, 1, dzb, w3b),
        first_two: lambda: (load_n1[0].wait(), grad_act(6, 0, 0, dub, w2b)),
        first_two + 1: lambda: (load_n1[1].wait(), grad_act(7, 1, 0, dub, w2b)),
        first_two + 2: lambda: grad_pre(6, 0, 0, du1),
        first_two + 3: lambda: (grad_pre(7, 1, 0, du1), [cp.start() for cp in load_h(first_one)]),
    }

    def weight_tick(t):
        for cp in load_h(t):
            cp.wait()
        if not isinstance(t, int) or t + 1 < COUNT:
            for cp in load_h(t + 1):
                cp.start()
        weight_grad(t, x2.at[:, lanes(lax.rem(t, 2) * CHUNK, chunk_of(t)[1])], du1)

    for t in range(first_one):
        chunks.steps(t)
        if t == first_two:
            for v in (0, 1):
                grad_pre(4 + v, v, 1, dub)
                load_n1[v].start()
        row, size = chunk_of(t)
        if not t:
            chunks.part_of(t)[...] = chunks.part_of(t)[...] + dot(x2[view[1], lead], dzb[view[1], :], TN)
            chunks.reduce(t).begin()
        elif t < first_two:
            weight_grad(t, x2.at[:, lanes(row, size)], dzb)
        else:
            weight_grad(t, x1.at[:, lanes(row - dim, size)], dub)
        if t in extra:
            extra[t]()

    def tick(t):
        chunks.steps(t)
        weight_tick(t)

    last_even = LEAD + EVEN - 1
    loop(last_even - first_one, lambda i: tick(first_one + i))
    for t in range(last_even, COUNT + LAST_STEP):
        chunks.steps(t)
        if t < COUNT:
            weight_tick(t)
    loss_o[...] = jnp.broadcast_to(jnp.sum(lstats.total(0)) + 2.0 * sq_sum / all_rows, loss_o.shape)
    for ex in (stats, zstats, lstats):
        ex.drain()
    for red in (a0, a1, b0, b1):
        red.drain_full()


def train_step(n_dev, h_a, h_b, w1, w2, w3, *affine):
    rows, feat = h_a.shape
    dim = w2.shape[0]
    total = 2 * dim + feat
    any_spec = pl.BlockSpec(memory_space=pl.ANY)
    vm = pl.BlockSpec(memory_space=pltpu.VMEM)
    dma = pltpu.SemaphoreType.DMA
    wide = (2 * rows, dim)
    moments = (2, dim)
    return pl.pallas_call(
        functools.partial(step_kernel, rows * n_dev),
        name='train_step',
        out_shape=[pltpu.VMEM((total, dim), F32), pltpu.VMEM((4, dim), F32), pltpu.VMEM((1, LANES), F32), jax.ShapeDtypeStruct(wide, F32)],
        in_specs=[any_spec] * 5 + [vm] * 4,
        out_specs=[vm] * 3 + [any_spec],
        scratch_shapes=[
            pltpu.VMEM((2 * rows, feat), BF16), pltpu.VMEM((feat, dim), BF16), pltpu.VMEM((dim, dim), BF16), pltpu.VMEM((dim, dim), BF16),
            pltpu.VMEM(wide, BF16), pltpu.VMEM(wide, BF16), pltpu.VMEM(wide, F32), pltpu.VMEM((2, PACKED, BLK), BF16),
            pltpu.VMEM((PART_SLOTS * CHUNK, dim), F32), pltpu.VMEM((CORE_SLOTS * CHUNK // 2 + LINK_SLOTS * CHUNK * 3 // 8, dim), F32),
            pltpu.VMEM((4, dim), F32),
            pltpu.VMEM((8,) + moments, F32), pltpu.VMEM((8, NDEV) + moments, F32),
            pltpu.VMEM((1, 4, dim), F32), pltpu.VMEM((1, NDEV, 4, dim), F32),
            pltpu.VMEM((1, 1, LANES), F32), pltpu.VMEM((1, NDEV, 1, LANES), F32),
            dma((5,)), dma((2,)), dma((2, 2)), dma((8, NDEV)), dma((8, NDEV)), dma((1, NDEV)), dma((1, NDEV)), dma((1, NDEV)), dma((1, NDEV)),
            dma((2, 2, 10)), dma((2, 2, 10)), dma((COUNT, 10)), dma((COUNT, 10))],
        compiler_params=pltpu.CompilerParams(collective_id=0, has_side_effects=True, vmem_limit_bytes=VMEM_BYTES - total * dim * 4 - SPARE),
    )(h_a, h_b, w1, w2, w3, *affine)


def emit_kernel(rows, grads, bn, loss, *refs):
    big, small, (sem,) = refs[:3], refs[3:8], refs[8:]
    copies = [pltpu.make_async_copy(grads.at[pl.ds(lo, hi - lo)], dst, sem.at[i]) for i, (dst, (lo, hi)) in enumerate(zip(big, rows))]
    for cp in copies:
        cp.start()
    for i in range(4):
        small[i][...] = bn[one(i), :]
    small[4][...] = loss[...]
    for cp in copies:
        cp.wait()


def emit(grads, bn, loss, dim):
    total = grads.shape[0]
    rows = ((2 * dim, total), (dim, 2 * dim), (0, dim))
    any_spec = pl.BlockSpec(memory_space=pl.ANY)
    vm = pl.BlockSpec(memory_space=pltpu.VMEM)
    vec = jax.ShapeDtypeStruct((1, dim), F32)
    return pl.pallas_call(
        functools.partial(emit_kernel, rows),
        name='emit',
        out_shape=[jax.ShapeDtypeStruct((hi - lo, dim), F32) for lo, hi in rows] + [vec] * 4 + [jax.ShapeDtypeStruct((1, LANES), F32)],
        in_specs=[vm, vm, vm],
        out_specs=[any_spec] * 3 + [vm] * 5,
        scratch_shapes=[pltpu.SemaphoreType.DMA((3,))],
        compiler_params=pltpu.CompilerParams(vmem_limit_bytes=VMEM_BYTES // 16),
    )(*(pltpu.with_memory_space_constraint(v, pltpu.VMEM) for v in (grads, bn, loss)))


def solution(mesh):
    n_dev = mesh.shape['data']

    def local_step(h_a, h_b, w_one, w_two, w_three, gain_one, bias_one, gain_two, bias_two):
        affine = [v.reshape(1, -1) for v in (gain_one, bias_one, gain_two, bias_two)]
        grads, bn, loss, _ = train_step(n_dev, h_a, h_b, w_one, w_two, w_three, *affine)
        d_one, d_two, d_three, *small, loss = emit(grads, bn, loss, w_two.shape[0])
        return (loss[0, 0], d_one, d_two, d_three) + tuple(v.reshape(-1) for v in small)

    row = P('data', None)
    return jax.shard_map(local_step, mesh=mesh, in_specs=(row, row) + (P(),) * 7, out_specs=(P(),) * 8, check_vma=False)
```

```python
import functools

import jax
import jax.numpy as jnp
from jax import lax
from jax.experimental import pallas as pl
from jax.experimental.pallas import tpu as pltpu
from jax.sharding import PartitionSpec as P

BN_EPS = 1e-5
STD_EPS = 1e-4
F32 = jnp.float32
BF16 = jnp.bfloat16
MESH = pl.DeviceIdType.MESH
NDEV = 8
BLK = 256
STRIP = 64
SPARE = 524288
ROWS = 512
VMEM_BYTES = 67043328
LANES = 128
QUAD = 128
DIAG_ROWS = 4 * QUAD
TRI_ROWS = 6 * QUAD
OFF_PAIRS = [(0, 1), (0, 2), (0, 3), (1, 2), (1, 3), (2, 3)]
PIECES = []
for _i in range(4):
    _b = _i * BLK
    PIECES += [(_i * QUAD, 0, _b, _b, QUAD, False), (_i * QUAD, QUAD, _b, _b + QUAD, QUAD, True),
               (DIAG_ROWS + _i // 2 * QUAD, _i % 2 * QUAD, _b + QUAD, _b + QUAD, QUAD, False)]
PIECES += [(TRI_ROWS + _b * BLK, 0, _i * BLK, _j * BLK, BLK, True) for _b, (_i, _j) in enumerate(OFF_PAIRS)]
PACKED = TRI_ROWS + len(OFF_PAIRS) * BLK
SPLIT = TRI_ROWS + 2 * BLK
SPANS = ((0, SPLIT), (SPLIT, PACKED))
ROW0, ROW1 = slice(0, 1), slice(1, 2)
TN = (((0,), (0,)), ((), ()))
NT = (((1,), (1,)), ((), ()))


def dot(a, b, dims=(((1,), (0,)), ((), ()))):
    return lax.dot_general(a, b, dims, preferred_element_type=F32)


def col_sum(v):
    return jnp.sum(v, axis=0, keepdims=True)


def one(i):
    return slice(i, i + 1)


def tile(j, size=BLK, base=0):
    return pl.ds(pl.multiple_of(base + j * size, size), size)


def span(i, base=0):
    return slice(base + i * BLK, base + i * BLK + BLK)


def loop(count, body):
    def step(i, carry):
        body(i)
        return carry

    lax.fori_loop(0, count, step, 0)


class Place:
    def __init__(self):
        me = lax.axis_index('data')
        self.me = me
        self.c = lax.rem(me, 2)
        self.x = lax.rem(me // 2, 2)
        self.y = me // 4

    def flip(self, dy, dx, dc):
        y = 1 - self.y if dy else self.y
        x = 1 - self.x if dx else self.x
        c = 1 - self.c if dc else self.c
        return y * 4 + x * 2 + c

    def peer(self, o):
        return self.flip(o & 4, o & 2, o & 1)


def greet(place):
    barrier = pltpu.get_barrier_semaphore()
    for o in range(1, NDEV):
        pl.semaphore_signal(barrier, inc=1, device_id=(place.peer(o),), device_id_type=MESH)


def meet():
    pl.semaphore_wait(pltpu.get_barrier_semaphore(), NDEV - 1)


class StatExchange:
    def __init__(self, place, src, rcv, ssem, rsem):
        self.place, self.src, self.rcv, self.ssem, self.rsem = place, src, rcv, ssem, rsem
        self.sent = []

    def copies(self, slot):
        place = self.place
        return [pltpu.make_async_remote_copy(
            src_ref=self.src.at[slot], dst_ref=self.rcv.at[slot, place.me],
            send_sem=self.ssem.at[slot, o], recv_sem=self.rsem.at[slot, o],
            device_id=(place.peer(o),), device_id_type=MESH) for o in range(1, NDEV)]

    def send(self, slot):
        self.rcv[slot, self.place.me] = self.src[slot]
        for cp in self.copies(slot):
            cp.start()
        self.sent.append(slot)

    def total(self, slot):
        for cp in self.copies(slot):
            cp.wait_recv()
        acc = self.rcv[slot, 0]
        for d in range(1, NDEV):
            acc = acc + self.rcv[slot, d]
        return acc

    def drain(self):
        for slot in self.sent:
            for cp in self.copies(slot):
                cp.wait_send()


class Reduce:
    def __init__(self, place, part, full, rc, r1, r2, ssem, rsem):
        self.place, self.part, self.full = place, part, full
        self.ssem, self.rsem = ssem, rsem
        self.rows = part.shape[0]
        self.rc, self.r1, self.r2 = rc, r1, r2
        place_pq = [(place.x, place.y), (place.y, place.x)]
        rows, c = self.rows, place.c
        al = rows // 16
        self.leaf_rows = al
        mo = lambda v: pl.multiple_of(v, al)
        self.half_mine = mo(c * (rows // 2))
        self.half_other = mo((1 - c) * (rows // 2))
        self.o1_mine, self.o1_other, self.o2_mine, self.o2_other = [], [], [], []
        for k, (p, q) in enumerate(place_pq):
            base = c * (rows // 2) + k * (rows // 4)
            self.o1_mine.append(mo(base + p * (rows // 8)))
            self.o1_other.append(mo(base + (1 - p) * (rows // 8)))
            self.o2_mine.append(mo(base + p * (rows // 8) + q * (rows // 16)))
            self.o2_other.append(mo(base + p * (rows // 8) + (1 - q) * (rows // 16)))
        self.dev_c = place.flip(0, 0, 1)
        self.dev_1 = [place.flip(0, 1, 0), place.flip(1, 0, 0)]
        self.dev_2 = [place.flip(1, 0, 0), place.flip(0, 1, 0)]

    def _cp(self, idx, src, dst, dev):
        return pltpu.make_async_remote_copy(src_ref=src, dst_ref=dst, send_sem=self.ssem.at[idx], recv_sem=self.rsem.at[idx],
                                            device_id=(dev,), device_id_type=MESH)

    def cp_c(self):
        return [self._cp(0, self.part.at[pl.ds(self.half_other, self.rows // 2)], self.rc, self.dev_c)]

    def cp_1(self):
        return [self._cp(1 + k, self.part.at[pl.ds(self.o1_other[k], self.rows // 8)], self.r1[k], self.dev_1[k]) for k in (0, 1)]

    def cp_2(self):
        return [self._cp(3 + k, self.part.at[pl.ds(self.o2_other[k], self.rows // 16)], self.r2[k], self.dev_2[k]) for k in (0, 1)]

    def cp_g2(self):
        return [self._cp(5 + k, self.full.at[pl.ds(self.o2_mine[k], self.rows // 16)],
                         self.full.at[pl.ds(self.o2_mine[k], self.rows // 16)], self.dev_2[k]) for k in (0, 1)]

    def cp_g1(self):
        return [self._cp(7 + k, self.full.at[pl.ds(self.o1_mine[k], self.rows // 8)],
                         self.full.at[pl.ds(self.o1_mine[k], self.rows // 8)], self.dev_1[k]) for k in (0, 1)]

    def cp_gc(self):
        half = pl.ds(self.half_mine, self.rows // 2)
        return [self._cp(9, self.full.at[half], self.full.at[half], self.dev_c)]

    @staticmethod
    def start(cps):
        for cp in cps:
            cp.start()

    def begin(self):
        self.start(self.cp_c())

    def step_1(self):
        self.cp_c()[0].wait_recv()
        mine = pl.ds(self.half_mine, self.rows // 2)
        self.part[mine] = self.part[mine] + self.rc[...]
        self.start(self.cp_1())

    def step_2(self):
        for k, (cp, nxt) in enumerate(zip(self.cp_1(), self.cp_2())):
            cp.wait_recv()
            mine = pl.ds(self.o1_mine[k], self.rows // 8)
            self.part[mine] = self.part[mine] + self.r1[k][...]
            nxt.start()

    def step_3(self, finish):
        for k, (cp, nxt) in enumerate(zip(self.cp_2(), self.cp_g2())):
            cp.wait_recv()
            mine = pl.ds(self.o2_mine[k], self.rows // 16)
            self.full[mine] = finish(self.o2_mine[k], self.part[mine] + self.r2[k][...])
            nxt.start()

    def step_4(self):
        for cp in self.cp_g2():
            cp.wait_recv()
        self.start(self.cp_g1())

    def step_5(self):
        for cp in self.cp_g1():
            cp.wait_recv()
        self.start(self.cp_gc())

    def step_6(self):
        self.cp_gc()[0].wait_recv()

    def drain_part(self):
        for cp in self.cp_c() + self.cp_1() + self.cp_2():
            cp.wait_send()

    def drain_full(self):
        for cp in self.cp_g2() + self.cp_g1() + self.cp_gc():
            cp.wait_send()


def by_rows(lhs, rhs, use, sums=0, dims=(((1,), (0,)), ((), ()))):
    def step(i, carry):
        rws = tile(i, ROWS)
        terms = use(rws, dot(lhs[rws, :], rhs[...], dims))
        return tuple(c + col_sum(t) for c, t in zip(carry, terms))

    width = rhs.shape[1 - dims[0][1][0]]
    return lax.fori_loop(0, lhs.shape[0] // ROWS, step, (jnp.zeros((1, width), F32),) * sums)


CHUNK, SMALL = 256, 128
LEAD, EVEN, TAIL = 0, 16, 0
COUNT = LEAD + EVEN + TAIL
PART_SLOTS, CORE_SLOTS, LINK_SLOTS = 3, 3, 4
LAST_STEP = 6


def chunk_of(t):
    if not isinstance(t, int) or LEAD <= t < LEAD + EVEN:
        return (t - LEAD) * CHUNK + LEAD * SMALL, CHUNK
    if t < LEAD:
        return t * SMALL, SMALL
    return EVEN * CHUNK + (t - EVEN) * SMALL, SMALL


class Chunks:
    def __init__(self, place, part, net, out, ssem, rsem):
        self.place, self.part, self.net, self.out = place, part, net, out
        self.ssem, self.rsem = ssem, rsem

    def reduce(self, t):
        row, size = chunk_of(t)
        link = lax.rem(t, LINK_SLOTS)

        def landing(base, slot, room, used):
            return self.net.at[pl.ds(pl.multiple_of(base + slot * room, 8), used)]

        one_base = CORE_SLOTS * CHUNK // 2
        two_base = one_base + LINK_SLOTS * CHUNK // 4
        return Reduce(self.place, self.part_of(t), self.out.at[pl.ds(pl.multiple_of(row, SMALL), size)],
                      landing(0, lax.rem(t, CORE_SLOTS), CHUNK // 2, size // 2),
                      [landing(one_base, 2 * link + k, CHUNK // 8, size // 8) for k in (0, 1)],
                      [landing(two_base, 2 * link + k, CHUNK // 16, size // 16) for k in (0, 1)], self.ssem.at[t], self.rsem.at[t])

    def part_of(self, t):
        return self.part.at[pl.ds(pl.multiple_of(lax.rem(t, PART_SLOTS) * CHUNK, CHUNK), chunk_of(t)[1])]

    def step(self, k, t):
        red = self.reduce(t)
        if k == 3:
            red.step_3(lambda row, acc: acc)
            red.drain_part()
        else:
            getattr(red, 'step_%d' % k)()
        if k == LAST_STEP:
            red.drain_full()

    def steps(self, t, first=1, last=LAST_STEP):
        for k in range(first, last + 1):
            if not isinstance(t, int) or 0 <= t - k < COUNT:
                self.step(k, t - k)


GramReduce = Reduce


def step_kernel(all_rows, h_a, h_b, w1, w2, w3, g1, b1, g2, b2,
                grads, bn_o, loss_o, n1_o,
                affine_b, hbuf, w1b, w2b, w3b, x1, x2, nb, ghat, part, net, invs,
                st_src, st_rcv, zs_src, zs_rcv, ls_src, ls_rcv,
                ld_sem, n_sem, h_sem, st_ss, st_rs, zs_ss, zs_rs, ls_ss, ls_rs, gr_ss, gr_rs, rd_ss, rd_rs):
    dim = w2b.shape[0]
    rows, feat = h_a.shape
    affine = ((affine_b.at[0], affine_b.at[1]), (affine_b.at[2], affine_b.at[3]))
    view = [slice(0, rows), slice(rows, 2 * rows)]
    low, high = slice(0, 2 * dim), slice(2 * dim, 2 * dim + feat)
    u1, dxb = grads.at[low], grads.at[high]
    place = Place()
    greet(place)
    h_all = (h_a, h_b)
    strip = lambda i: slice(i * ROWS, i * ROWS + ROWS)
    loads = {}
    for name, src, dst in (('w1', w1, w1b), *(('ha%d' % i, h_a.at[strip(i)], hbuf.at[strip(i)]) for i in range(rows // ROWS)), ('hb', h_b, hbuf.at[view[1]]), ('w2', w2, w2b), ('w3', w3, w3b),
                           *(('affine%d' % i, src, affine_b.at[i]) for i, src in enumerate((g1, b1, g2, b2)))):
        loads[name] = pltpu.make_async_copy(src, dst, ld_sem.at[len(loads)])
        loads[name].start()
    spill = [pltpu.make_async_copy(u1.at[view[v]], n1_o.at[view[v]], n_sem.at[v]) for v in (0, 1)]
    load_n1 = [pltpu.make_async_copy(n1_o.at[view[v]], nb.at[view[v]], n_sem.at[v]) for v in (0, 1)]

    def lanes(row, size):
        return pl.ds(pl.multiple_of(row, SMALL), size)

    stats = StatExchange(place, st_src, st_rcv, st_ss, st_rs)
    zstats = StatExchange(place, zs_src, zs_rcv, zs_ss, zs_rs)
    lstats = StatExchange(place, ls_src, ls_rcv, ls_ss, ls_rs)

    def linear(slot, dst, lhs, rhs):
        def use(rws, out):
            dst[rws, :] = out
            return out, out * out

        if slot:
            sums = by_rows(lhs, rhs, use, 2)
        else:
            sums = None
            for i in range(rows // ROWS):
                loads['ha%d' % i].wait()
                out = dot(lhs[strip(i), :], rhs[...])
                terms = [col_sum(t) for t in use(strip(i), out)]
                sums = [a + b for a, b in zip(sums, terms)] if i else terms
            meet()
        st_src[slot, ROW0, :], st_src[slot, ROW1, :] = sums
        stats.send(slot)

    def norm_relu(slot, v, layer, ubuf, xbuf):
        mom = stats.total(slot)
        mean = mom[ROW0] / all_rows
        var = mom[ROW1] / all_rows - mean * mean
        inv = lax.rsqrt(var + BN_EPS)
        invs[one(slot), :] = inv
        gain, bias = affine[layer]

        def body(i):
            rws = tile(i, STRIP, v * rows)
            n = (ubuf[rws, :] - mean) * inv
            ubuf[rws, :] = n
            xbuf[rws, :] = jnp.maximum(gain[...] * n + bias[...], 0.0).astype(BF16)

        loop(rows // STRIP, body)

    zcol = pl.ds(dim, dim)
    dzb = hbuf.at[:, pl.ds(0, dim)]
    zb = [hbuf.at[view[v], zcol] for v in (0, 1)]

    def project(v):
        def use(rws, out):
            z = out.astype(BF16)
            zb[v][rws, :] = z
            zf = z.astype(F32)
            if not v:
                return zf,
            diff = zb[0][rws, :].astype(F32) - zf
            return zf, diff * diff

        for o, term in enumerate(by_rows(x2.at[view[v]], w3b, use, 1 + v)):
            zs_src[0, one(v + o), :] = term

    outer, gram = grads.at[low], grads.at[high]

    def band(v, ch):
        return pl.ds((2 * v + ch) * BLK, BLK)

    def packed_at(ref, v, row, lane, size):
        ch = int(row >= SPLIT)
        return ref.at[pl.ds(row - SPANS[ch][0], size), pl.ds((2 * v + ch) * BLK + lane, size)]

    gram_at = functools.partial(packed_at, gram)

    def gram_of(v, chunk):
        if not chunk:
            for i in range(dim // BLK):
                zi = hbuf[view[v], span(i, dim)]
                sq = dot(zi, zi, TN)
                for row, lane, r, c, size, _ in PIECES[3 * i:3 * i + 3]:
                    gram_at(v, row, lane, size)[...] = sq[r - i * BLK:r - i * BLK + size, c - i * BLK:c - i * BLK + size]
        lo, hi = SPANS[chunk]
        for b, (i, j) in enumerate(OFF_PAIRS):
            row = TRI_ROWS + b * BLK
            if lo <= row < hi:
                gram_at(v, row, 0, BLK)[...] = dot(hbuf[view[v], span(i, dim)], hbuf[view[v], span(j, dim)], TN)
        reds[v][chunk].begin()

    reds = []
    for v in (0, 1):
        pair = []
        for ch, (lo, hi) in enumerate(SPANS):
            n, bd = hi - lo, band(v, ch)
            r1 = [net.at[pl.ds(k * n // 8, n // 8), bd] for k in (0, 1)]
            r2 = [net.at[pl.ds(n // 4 + k * n // 16, n // 16), bd] for k in (0, 1)]
            pair.append(GramReduce(place, gram.at[pl.ds(0, n), bd], ghat.at[v, pl.ds(lo, n)], part.at[pl.ds(0, n // 2), bd], r1, r2,
                                   gr_ss.at[v, ch], gr_rs.at[v, ch]))
        reds.append(pair)
    (a0, a1), (b0, b1) = reds

    def store_outer(mus):
        for v in (0, 1):
            for row, lane, r, c, size, _ in PIECES:
                col = jnp.transpose(jnp.broadcast_to(mus[v][:, r:r + size], (size, size)))
                packed_at(outer, v, row, lane, size)[...] = (all_rows * col) * mus[v][:, c:c + size]

    def finish(v, ch):
        def fin(row, acc):
            leaf = acc.shape[0]
            prow = SPANS[ch][0] + row + lax.broadcasted_iota(jnp.int32, acc.shape, 0)
            lane = lax.broadcasted_iota(jnp.int32, acc.shape, 1)
            quad = (prow < TRI_ROWS) & ((prow >= DIAG_ROWS) | (lane < QUAD))
            eye = quad & (lax.rem(prow, QUAD) == lax.rem(lane, QUAD))
            cov = (acc - outer[pl.ds(row, leaf), band(v, ch)]) / (all_rows - 1)
            std = jnp.sqrt(cov + STD_EPS)
            hinge = jnp.where(eye, jnp.maximum(1.0 - std, 0.0), 0.0)
            off = jnp.where(eye, 0.0, cov * cov) * jnp.where(quad, 1.0, 2.0)
            term = col_sum(hinge + 2.0 * off)
            ls_src[0] = ls_src[0] + term[:, :LANES] + term[:, LANES:]
            on = jnp.where(std < 1.0, 1.0, 0.0)
            return jnp.where(eye, -on / (2.0 * std), 4.0 * cov).astype(BF16)
        return fin

    def expand(v):
        for row, lane, r, c, size, mirrored in PIECES:
            blk = ghat[v, row:row + size, lane:lane + size]
            w1b[v * dim + r:v * dim + r + size, c:c + size] = blk
            if mirrored:
                w1b[v * dim + c:v * dim + c + size, r:r + size] = jnp.transpose(blk)

    def grad_z(v, mu, between):
        hi = mu.astype(BF16)
        mid = (mu - hi.astype(F32)).astype(BF16)
        low = (mu - hi.astype(F32) - mid.astype(F32)).astype(BF16)
        parts = jnp.concatenate([hi, mid, low, jnp.zeros((13, dim), BF16)], axis=0)
        g = w1b.at[pl.ds(v * dim, dim)]
        mean_part = col_sum(dot(parts, g[...]))
        sign = -1.0 if v else 1.0

        for part in range(rows // ROWS):
            sub = pl.ds(part * ROWS, ROWS)
            za, zo, out = zb[0].at[sub], zb[1].at[sub], dzb.at[pl.ds(v * rows + part * ROWS, ROWS)]

            def use(rws, row_part):
                diff = za[rws, :].astype(F32) - zo[rws, :].astype(F32)
                dz = (2.0 / (all_rows - 1)) * (row_part - mean_part) + (sign * 4.0 / all_rows) * diff
                out[rws, :] = dz.astype(BF16)
                return ()

            by_rows(zb[v].at[sub], g, use)
            if between:
                between.pop(0)()

    chunks = Chunks(place, part, net, grads, rd_ss, rd_rs)

    def load_h(t):
        row, size = chunk_of(t)
        slot = lax.rem(t, 2)
        return [pltpu.make_async_copy(h.at[:, lanes(row - 2 * dim, size)], x2.at[view[v], lanes(slot * CHUNK, size)], h_sem.at[slot, v])
                for v, h in enumerate(h_all)]

    def weight_grad(t, lhs, rhs):
        dst = chunks.part_of(t)

        def half(j):
            cols = tile(j, ROWS)
            dst[:, cols] = dot(lhs[...], rhs[:, cols], TN)

        loop(dim // ROWS, half)
        chunks.reduce(t).begin()

    def grad_act(slot, v, layer, src, w):
        gain, bias = affine[layer]
        n_ref, dst = nb.at[view[v]], dxb.at[view[v]]

        def use(rws, dx):
            n = n_ref[rws, :]
            da = jnp.where(gain[...] * n + bias[...] > 0.0, dx, 0.0)
            dst[rws, :] = da
            return da, da * n

        st_src[slot, ROW0, :], st_src[slot, ROW1, :] = by_rows(src.at[view[v]], w, use, 2, NT)
        stats.send(slot)

    def grad_pre(slot, v, layer, dst):
        sums = stats.total(slot)
        for row, o in ((ROW1, 2 * layer), (ROW0, 2 * layer + 1)):
            bn_o[one(o), :] = bn_o[one(o), :] + sums[row] if v else sums[row]
        mean_d = sums[ROW0] / all_rows
        mean_dn = sums[ROW1] / all_rows
        scale = invs[one(2 * layer + v), :] * affine[layer][0][...]

        def body(i):
            rws = tile(i, STRIP, v * rows)
            dst[rws, :] = (scale * (dxb[rws, :] - mean_d - nb[rws, :] * mean_dn)).astype(BF16)

        loop(rows // STRIP, body)

    loads['w1'].wait()
    linear(0, u1.at[view[0]], hbuf.at[view[0]], w1b)
    loads['hb'].wait()
    linear(1, u1.at[view[1]], hbuf.at[view[1]], w1b)
    for name in list(loads):
        if name[0] not in 'h1' and name != 'w1':
            loads[name].wait()
    for v in (0, 1):
        norm_relu(v, v, 0, u1, x1)
        spill[v].start()
        linear(2 + v, nb.at[view[v]], x1.at[view[v]], w2b)
    zs_src[0] = jnp.zeros(zs_src.shape[1:], F32)
    ls_src[0] = jnp.zeros((1, LANES), F32)
    norm_relu(2, 0, 1, nb, x2)
    project(0)
    gram_of(0, 0)
    gram_of(0, 1)
    norm_relu(3, 1, 1, nb, x2)
    a0.step_1()
    a1.step_1()
    project(1)
    zstats.send(0)
    gram_of(1, 0)
    gram_of(1, 1)
    a0.step_2()
    b0.step_1()
    b1.step_1()
    a1.step_2()
    ztot = zstats.total(0)
    mus = [ztot[one(v)] / all_rows for v in (0, 1)]
    sq_sum = jnp.sum(ztot[one(2)])
    for cp in spill:
        cp.wait()
    store_outer(mus)
    a0.step_3(finish(0, 0))
    a1.step_3(finish(0, 1))
    b0.step_2()
    a0.step_4()
    b1.step_2()
    a1.step_4()
    b0.step_3(finish(1, 0))
    b1.step_3(finish(1, 1))
    lstats.send(0)
    b0.step_4()
    a0.step_5()
    b1.step_4()
    a1.step_5()
    a0.step_6()
    a1.step_6()
    expand(0)
    grad_z(0, mus[0], [b0.step_5])
    lead = lanes(0, chunk_of(0)[1])
    chunks.part_of(0)[...] = dot(x2[view[0], lead], dzb[view[0], :], TN)
    b1.step_5()
    b0.step_6()
    b1.step_6()
    expand(1)
    grad_z(1, mus[1], [])
    for red in (a0, a1, b0, b1):
        red.drain_part()

    dub, du1 = w1b, hbuf.at[:, zcol]
    first_two = next(t for t in range(COUNT) if chunk_of(t)[0] >= dim)
    first_one = next(t for t in range(COUNT) if chunk_of(t)[0] >= 2 * dim)
    extra = {
        first_two - 2: lambda: grad_act(4, 0, 1, dzb, w3b),
        first_two - 1: lambda: grad_act(5, 1, 1, dzb, w3b),
        first_two: lambda: (load_n1[0].wait(), grad_act(6, 0, 0, dub, w2b)),
        first_two + 1: lambda: (load_n1[1].wait(), grad_act(7, 1, 0, dub, w2b)),
        first_two + 2: lambda: grad_pre(6, 0, 0, du1),
        first_two + 3: lambda: (grad_pre(7, 1, 0, du1), [cp.start() for cp in load_h(first_one)]),
    }

    def weight_tick(t):
        for cp in load_h(t):
            cp.wait()
        if not isinstance(t, int) or t + 1 < COUNT:
            for cp in load_h(t + 1):
                cp.start()
        weight_grad(t, x2.at[:, lanes(lax.rem(t, 2) * CHUNK, chunk_of(t)[1])], du1)

    for t in range(first_one):
        early = t < PART_SLOTS
        chunks.steps(t, 1, t - 1 if early else LAST_STEP)
        if t == first_two:
            for v in (0, 1):
                grad_pre(4 + v, v, 1, dub)
                load_n1[v].start()
        row, size = chunk_of(t)
        if not t:
            chunks.part_of(t)[...] = chunks.part_of(t)[...] + dot(x2[view[1], lead], dzb[view[1], :], TN)
            chunks.reduce(t).begin()
        elif t < first_two:
            weight_grad(t, x2.at[:, lanes(row, size)], dzb)
        else:
            weight_grad(t, x1.at[:, lanes(row - dim, size)], dub)
        if early:
            chunks.steps(t, max(t, 1))
        if t in extra:
            extra[t]()

    def tick(t):
        chunks.steps(t)
        weight_tick(t)

    last_even = LEAD + EVEN - 1
    loop(last_even - first_one, lambda i: tick(first_one + i))
    for t in range(last_even, COUNT + LAST_STEP):
        chunks.steps(t)
        if t < COUNT:
            weight_tick(t)
    loss_o[...] = jnp.broadcast_to(jnp.sum(lstats.total(0)) + 2.0 * sq_sum / all_rows, loss_o.shape)
    for ex in (stats, zstats, lstats):
        ex.drain()
    for red in (a0, a1, b0, b1):
        red.drain_full()


def train_step(n_dev, h_a, h_b, w1, w2, w3, *affine):
    rows, feat = h_a.shape
    dim = w2.shape[0]
    total = 2 * dim + feat
    any_spec = pl.BlockSpec(memory_space=pl.ANY)
    vm = pl.BlockSpec(memory_space=pltpu.VMEM)
    dma = pltpu.SemaphoreType.DMA
    wide = (2 * rows, dim)
    moments = (2, dim)
    return pl.pallas_call(
        functools.partial(step_kernel, rows * n_dev),
        name='train_step',
        out_shape=[pltpu.VMEM((total, dim), F32), pltpu.VMEM((4, dim), F32), pltpu.VMEM((1, LANES), F32), jax.ShapeDtypeStruct(wide, F32)],
        in_specs=[any_spec] * 9,
        out_specs=[vm] * 3 + [any_spec],
        scratch_shapes=[
            pltpu.VMEM((4, 1, dim), F32), pltpu.VMEM((2 * rows, feat), BF16), pltpu.VMEM((feat, dim), BF16), pltpu.VMEM((dim, dim), BF16), pltpu.VMEM((dim, dim), BF16),
            pltpu.VMEM(wide, BF16), pltpu.VMEM(wide, BF16), pltpu.VMEM(wide, F32), pltpu.VMEM((2, PACKED, BLK), BF16),
            pltpu.VMEM((PART_SLOTS * CHUNK, dim), F32), pltpu.VMEM((CORE_SLOTS * CHUNK // 2 + LINK_SLOTS * CHUNK * 3 // 8, dim), F32),
            pltpu.VMEM((4, dim), F32),
            pltpu.VMEM((8,) + moments, F32), pltpu.VMEM((8, NDEV) + moments, F32),
            pltpu.VMEM((1, 4, dim), F32), pltpu.VMEM((1, NDEV, 4, dim), F32),
            pltpu.VMEM((1, 1, LANES), F32), pltpu.VMEM((1, NDEV, 1, LANES), F32),
            dma((8 + rows // ROWS,)), dma((2,)), dma((2, 2)), dma((8, NDEV)), dma((8, NDEV)), dma((1, NDEV)), dma((1, NDEV)), dma((1, NDEV)), dma((1, NDEV)),
            dma((2, 2, 10)), dma((2, 2, 10)), dma((COUNT, 10)), dma((COUNT, 10))],
        compiler_params=pltpu.CompilerParams(collective_id=0, has_side_effects=True, vmem_limit_bytes=VMEM_BYTES - total * dim * 4 - SPARE),
    )(h_a, h_b, w1, w2, w3, *affine)


def emit_kernel(rows, grads, bn, loss, *refs):
    outs, sem = refs[:-1], refs[-1]
    srcs = [grads.at[pl.ds(lo, hi - lo)] for lo, hi in rows] + [bn.at[one(i)] for i in range(4)] + [loss]
    copies = [pltpu.make_async_copy(src, dst, sem.at[i]) for i, (src, dst) in enumerate(zip(srcs, outs))]
    for cp in copies:
        cp.start()
    for cp in copies:
        cp.wait()


def emit(grads, bn, loss, dim):
    total = grads.shape[0]
    rows = ((2 * dim, total), (dim, 2 * dim), (0, dim))
    any_spec = pl.BlockSpec(memory_space=pl.ANY)
    vm = pl.BlockSpec(memory_space=pltpu.VMEM)
    vec = jax.ShapeDtypeStruct((1, dim), F32)
    return pl.pallas_call(
        functools.partial(emit_kernel, rows),
        name='emit',
        out_shape=[jax.ShapeDtypeStruct((hi - lo, dim), F32) for lo, hi in rows] + [vec] * 4 + [jax.ShapeDtypeStruct((1, LANES), F32)],
        in_specs=[vm, vm, vm],
        out_specs=[any_spec] * 8,
        scratch_shapes=[pltpu.SemaphoreType.DMA((8,))],
        compiler_params=pltpu.CompilerParams(vmem_limit_bytes=VMEM_BYTES // 16),
    )(*(pltpu.with_memory_space_constraint(v, pltpu.VMEM) for v in (grads, bn, loss)))


def solution(mesh):
    n_dev = mesh.shape['data']

    def local_step(h_a, h_b, w_one, w_two, w_three, gain_one, bias_one, gain_two, bias_two):
        affine = [v.reshape(1, -1) for v in (gain_one, bias_one, gain_two, bias_two)]
        grads, bn, loss, _ = train_step(n_dev, h_a, h_b, w_one, w_two, w_three, *affine)
        d_one, d_two, d_three, *small, loss = emit(grads, bn, loss, w_two.shape[0])
        return (loss[0, 0], d_one, d_two, d_three) + tuple(v.reshape(-1) for v in small)

    row = P('data', None)
    return jax.shard_map(local_step, mesh=mesh, in_specs=(row, row) + (P(),) * 7, out_specs=(P(),) * 8, check_vma=False)
```

```python
import functools

import jax
import jax.numpy as jnp
from jax import lax
from jax.experimental import pallas as pl
from jax.experimental.pallas import tpu as pltpu
from jax.sharding import PartitionSpec as P

BN_EPS = 1e-5
STD_EPS = 1e-4
F32 = jnp.float32
BF16 = jnp.bfloat16
MESH = pl.DeviceIdType.MESH
NDEV = 8
BLK = 256
STRIP = 64
SETS = 4
SPARE = 524288
ROWS = 512
VMEM_BYTES = 67043328
LANES = 128
QUAD = 128
DIAG_ROWS = 4 * QUAD
TRI_ROWS = 6 * QUAD
OFF_PAIRS = [(0, 1), (0, 2), (0, 3), (1, 2), (1, 3), (2, 3)]
PIECES = []
for _i in range(4):
    _b = _i * BLK
    PIECES += [(_i * QUAD, 0, _b, _b, QUAD, False), (_i * QUAD, QUAD, _b, _b + QUAD, QUAD, True),
               (DIAG_ROWS + _i // 2 * QUAD, _i % 2 * QUAD, _b + QUAD, _b + QUAD, QUAD, False)]
PIECES += [(TRI_ROWS + _b * BLK, 0, _i * BLK, _j * BLK, BLK, True) for _b, (_i, _j) in enumerate(OFF_PAIRS)]
PACKED = TRI_ROWS + len(OFF_PAIRS) * BLK
SPLIT = TRI_ROWS + 2 * BLK
SPANS = ((0, SPLIT), (SPLIT, PACKED))
ROW0, ROW1 = slice(0, 1), slice(1, 2)
TN = (((0,), (0,)), ((), ()))
NT = (((1,), (1,)), ((), ()))


def dot(a, b, dims=(((1,), (0,)), ((), ()))):
    return lax.dot_general(a, b, dims, preferred_element_type=F32)


def col_sum(v):
    return jnp.sum(v, axis=0, keepdims=True)


def one(i):
    return slice(i, i + 1)


def tile(j, size=BLK, base=0):
    return pl.ds(pl.multiple_of(base + j * size, size), size)


def span(i, base=0):
    return slice(base + i * BLK, base + i * BLK + BLK)


def loop(count, body):
    def step(i, carry):
        body(i)
        return carry

    lax.fori_loop(0, count, step, 0)


class Place:
    def __init__(self):
        me = lax.axis_index('data')
        self.me = me
        self.c = lax.rem(me, 2)
        self.x = lax.rem(me // 2, 2)
        self.y = me // 4

    def flip(self, dy, dx, dc):
        y = 1 - self.y if dy else self.y
        x = 1 - self.x if dx else self.x
        c = 1 - self.c if dc else self.c
        return y * 4 + x * 2 + c

    def peer(self, o):
        return self.flip(o & 4, o & 2, o & 1)


def greet(place):
    barrier = pltpu.get_barrier_semaphore()
    for o in range(1, NDEV):
        pl.semaphore_signal(barrier, inc=1, device_id=(place.peer(o),), device_id_type=MESH)


def meet():
    pl.semaphore_wait(pltpu.get_barrier_semaphore(), NDEV - 1)


class StatExchange:
    def __init__(self, place, src, rcv, ssem, rsem):
        self.place, self.src, self.rcv, self.ssem, self.rsem = place, src, rcv, ssem, rsem
        self.sent = []

    def copies(self, slot):
        place = self.place
        return [pltpu.make_async_remote_copy(
            src_ref=self.src.at[slot], dst_ref=self.rcv.at[slot, place.me],
            send_sem=self.ssem.at[slot % SETS, o], recv_sem=self.rsem.at[slot % SETS, o],
            device_id=(place.peer(o),), device_id_type=MESH) for o in range(1, NDEV)]

    def send(self, slot):
        self.rcv[slot, self.place.me] = self.src[slot]
        for cp in self.copies(slot):
            cp.start()
        self.sent.append(slot)

    def total(self, slot):
        for cp in self.copies(slot):
            cp.wait_recv()
        acc = self.rcv[slot, 0]
        for d in range(1, NDEV):
            acc = acc + self.rcv[slot, d]
        return acc

    def drain(self):
        for slot in self.sent:
            for cp in self.copies(slot):
                cp.wait_send()
        self.sent = []


class Reduce:
    def __init__(self, place, part, full, rc, r1, r2, ssem, rsem):
        self.place, self.part, self.full = place, part, full
        self.ssem, self.rsem = ssem, rsem
        self.rows = part.shape[0]
        self.rc, self.r1, self.r2 = rc, r1, r2
        place_pq = [(place.x, place.y), (place.y, place.x)]
        rows, c = self.rows, place.c
        al = rows // 16
        self.leaf_rows = al
        mo = lambda v: pl.multiple_of(v, al)
        self.half_mine = mo(c * (rows // 2))
        self.half_other = mo((1 - c) * (rows // 2))
        self.o1_mine, self.o1_other, self.o2_mine, self.o2_other = [], [], [], []
        for k, (p, q) in enumerate(place_pq):
            base = c * (rows // 2) + k * (rows // 4)
            self.o1_mine.append(mo(base + p * (rows // 8)))
            self.o1_other.append(mo(base + (1 - p) * (rows // 8)))
            self.o2_mine.append(mo(base + p * (rows // 8) + q * (rows // 16)))
            self.o2_other.append(mo(base + p * (rows // 8) + (1 - q) * (rows // 16)))
        self.dev_c = place.flip(0, 0, 1)
        self.dev_1 = [place.flip(0, 1, 0), place.flip(1, 0, 0)]
        self.dev_2 = [place.flip(1, 0, 0), place.flip(0, 1, 0)]

    def _cp(self, idx, src, dst, dev):
        return pltpu.make_async_remote_copy(src_ref=src, dst_ref=dst, send_sem=self.ssem.at[idx], recv_sem=self.rsem.at[idx],
                                            device_id=(dev,), device_id_type=MESH)

    def cp_c(self):
        return [self._cp(0, self.part.at[pl.ds(self.half_other, self.rows // 2)], self.rc, self.dev_c)]

    def cp_1(self):
        return [self._cp(1 + k, self.part.at[pl.ds(self.o1_other[k], self.rows // 8)], self.r1[k], self.dev_1[k]) for k in (0, 1)]

    def cp_2(self):
        return [self._cp(3 + k, self.part.at[pl.ds(self.o2_other[k], self.rows // 16)], self.r2[k], self.dev_2[k]) for k in (0, 1)]

    def cp_g2(self):
        return [self._cp(5 + k, self.full.at[pl.ds(self.o2_mine[k], self.rows // 16)],
                         self.full.at[pl.ds(self.o2_mine[k], self.rows // 16)], self.dev_2[k]) for k in (0, 1)]

    def cp_g1(self):
        return [self._cp(7 + k, self.full.at[pl.ds(self.o1_mine[k], self.rows // 8)],
                         self.full.at[pl.ds(self.o1_mine[k], self.rows // 8)], self.dev_1[k]) for k in (0, 1)]

    def cp_gc(self):
        half = pl.ds(self.half_mine, self.rows // 2)
        return [self._cp(9, self.full.at[half], self.full.at[half], self.dev_c)]

    @staticmethod
    def start(cps):
        for cp in cps:
            cp.start()

    def begin(self):
        self.start(self.cp_c())

    def step_1(self):
        self.cp_c()[0].wait_recv()
        mine = pl.ds(self.half_mine, self.rows // 2)
        self.part[mine] = self.part[mine] + self.rc[...]
        self.start(self.cp_1())

    def step_2(self):
        for k, (cp, nxt) in enumerate(zip(self.cp_1(), self.cp_2())):
            cp.wait_recv()
            mine = pl.ds(self.o1_mine[k], self.rows // 8)
            self.part[mine] = self.part[mine] + self.r1[k][...]
            nxt.start()

    def step_3(self, finish):
        for k, (cp, nxt) in enumerate(zip(self.cp_2(), self.cp_g2())):
            cp.wait_recv()
            mine = pl.ds(self.o2_mine[k], self.rows // 16)
            self.full[mine] = finish(self.o2_mine[k], self.part[mine] + self.r2[k][...])
            nxt.start()

    def step_4(self):
        for cp in self.cp_g2():
            cp.wait_recv()
        self.start(self.cp_g1())

    def step_5(self):
        for cp in self.cp_g1():
            cp.wait_recv()
        self.start(self.cp_gc())

    def step_6(self):
        self.cp_gc()[0].wait_recv()

    def drain_part(self):
        for cp in self.cp_c() + self.cp_1() + self.cp_2():
            cp.wait_send()

    def drain_full(self):
        for cp in self.cp_g2() + self.cp_g1() + self.cp_gc():
            cp.wait_send()


def by_rows(lhs, rhs, use, sums=0, dims=(((1,), (0,)), ((), ()))):
    def step(i, carry):
        rws = tile(i, ROWS)
        terms = use(rws, dot(lhs[rws, :], rhs[...], dims))
        return tuple(c + col_sum(t) for c, t in zip(carry, terms))

    width = rhs.shape[1 - dims[0][1][0]]
    return lax.fori_loop(0, lhs.shape[0] // ROWS, step, (jnp.zeros((1, width), F32),) * sums)


CHUNK, SMALL = 256, 128
LEAD, EVEN, TAIL = 0, 16, 0
COUNT = LEAD + EVEN + TAIL
PART_SLOTS, CORE_SLOTS, LINK_SLOTS = 3, 3, 4
LAST_STEP = 6


def chunk_of(t):
    if not isinstance(t, int) or LEAD <= t < LEAD + EVEN:
        return (t - LEAD) * CHUNK + LEAD * SMALL, CHUNK
    if t < LEAD:
        return t * SMALL, SMALL
    return EVEN * CHUNK + (t - EVEN) * SMALL, SMALL


class Chunks:
    def __init__(self, place, part, net, out, ssem, rsem):
        self.place, self.part, self.net, self.out = place, part, net, out
        self.ssem, self.rsem = ssem, rsem

    def reduce(self, t):
        row, size = chunk_of(t)
        link = lax.rem(t, LINK_SLOTS)

        def landing(base, slot, room, used):
            return self.net.at[pl.ds(pl.multiple_of(base + slot * room, 8), used)]

        one_base = CORE_SLOTS * CHUNK // 2
        two_base = one_base + LINK_SLOTS * CHUNK // 4
        return Reduce(self.place, self.part_of(t), self.out.at[pl.ds(pl.multiple_of(row, SMALL), size)],
                      landing(0, lax.rem(t, CORE_SLOTS), CHUNK // 2, size // 2),
                      [landing(one_base, 2 * link + k, CHUNK // 8, size // 8) for k in (0, 1)],
                      [landing(two_base, 2 * link + k, CHUNK // 16, size // 16) for k in (0, 1)], self.ssem.at[lax.rem(t, SETS)], self.rsem.at[lax.rem(t, SETS)])

    def part_of(self, t):
        return self.part.at[pl.ds(pl.multiple_of(lax.rem(t, PART_SLOTS) * CHUNK, CHUNK), chunk_of(t)[1])]

    def step(self, k, t):
        red = self.reduce(t)
        if k == 3:
            red.step_3(lambda row, acc: acc)
            red.drain_part()
        else:
            getattr(red, 'step_%d' % k)()
        if k == LAST_STEP:
            red.drain_full()

    def steps(self, t, first=1, last=LAST_STEP):
        for k in range(first, last + 1):
            if not isinstance(t, int) or 0 <= t - k < COUNT:
                self.step(k, t - k)


GramReduce = Reduce


def step_kernel(all_rows, h_a, h_b, w1, w2, w3, g1, b1, g2, b2,
                grads, bn_o, loss_o, n1_o,
                affine_b, hbuf, w1b, w2b, w3b, x1, x2, nb, ghat, part, net, invs,
                st_src, st_rcv, zs_src, zs_rcv, ls_src, ls_rcv,
                ld_sem, n_sem, h_sem, st_ss, st_rs, ls_ss, ls_rs, rd_ss, rd_rs):
    dim = w2b.shape[0]
    rows, feat = h_a.shape
    affine = ((affine_b.at[0], affine_b.at[1]), (affine_b.at[2], affine_b.at[3]))
    view = [slice(0, rows), slice(rows, 2 * rows)]
    low, high = slice(0, 2 * dim), slice(2 * dim, 2 * dim + feat)
    u1, dxb = grads.at[low], grads.at[high]
    place = Place()
    greet(place)
    h_all = (h_a, h_b)
    strip = lambda i: slice(i * ROWS, i * ROWS + ROWS)
    loads = {}
    for name, src, dst in (('w1', w1, w1b), *(('ha%d' % i, h_a.at[strip(i)], hbuf.at[strip(i)]) for i in range(rows // ROWS)), ('hb', h_b, hbuf.at[view[1]]), ('w2', w2, w2b), ('w3', w3, w3b),
                           *(('affine%d' % i, src, affine_b.at[i]) for i, src in enumerate((g1, b1, g2, b2)))):
        loads[name] = pltpu.make_async_copy(src, dst, ld_sem.at[len(loads)])
        loads[name].start()
    spill = [pltpu.make_async_copy(u1.at[view[v]], n1_o.at[view[v]], n_sem.at[v]) for v in (0, 1)]
    load_n1 = [pltpu.make_async_copy(n1_o.at[view[v]], nb.at[view[v]], n_sem.at[v]) for v in (0, 1)]

    def lanes(row, size):
        return pl.ds(pl.multiple_of(row, SMALL), size)

    stats = StatExchange(place, st_src, st_rcv, st_ss, st_rs)
    zstats = StatExchange(place, zs_src, zs_rcv, st_ss, st_rs)
    lstats = StatExchange(place, ls_src, ls_rcv, ls_ss, ls_rs)

    def linear(slot, dst, lhs, rhs):
        def use(rws, out):
            dst[rws, :] = out
            return out, out * out

        if slot:
            sums = by_rows(lhs, rhs, use, 2)
        else:
            sums = None
            for i in range(rows // ROWS):
                loads['ha%d' % i].wait()
                out = dot(lhs[strip(i), :], rhs[...])
                terms = [col_sum(t) for t in use(strip(i), out)]
                sums = [a + b for a, b in zip(sums, terms)] if i else terms
            meet()
        st_src[slot, ROW0, :], st_src[slot, ROW1, :] = sums
        stats.send(slot)

    def norm_relu(slot, v, layer, ubuf, xbuf):
        mom = stats.total(slot)
        mean = mom[ROW0] / all_rows
        var = mom[ROW1] / all_rows - mean * mean
        inv = lax.rsqrt(var + BN_EPS)
        invs[one(slot), :] = inv
        gain, bias = affine[layer]

        def body(i):
            rws = tile(i, STRIP, v * rows)
            n = (ubuf[rws, :] - mean) * inv
            ubuf[rws, :] = n
            xbuf[rws, :] = jnp.maximum(gain[...] * n + bias[...], 0.0).astype(BF16)

        loop(rows // STRIP, body)

    zcol = pl.ds(dim, dim)
    dzb = hbuf.at[:, pl.ds(0, dim)]
    zb = [hbuf.at[view[v], zcol] for v in (0, 1)]

    def project(v):
        def use(rws, out):
            z = out.astype(BF16)
            zb[v][rws, :] = z
            zf = z.astype(F32)
            if not v:
                return zf,
            diff = zb[0][rws, :].astype(F32) - zf
            return zf, diff * diff

        for o, term in enumerate(by_rows(x2.at[view[v]], w3b, use, 1 + v)):
            zs_src[0, one(v + o), :] = term

    outer, gram = grads.at[low], grads.at[high]

    def band(v, ch):
        return pl.ds((2 * v + ch) * BLK, BLK)

    def packed_at(ref, v, row, lane, size):
        ch = int(row >= SPLIT)
        return ref.at[pl.ds(row - SPANS[ch][0], size), pl.ds((2 * v + ch) * BLK + lane, size)]

    gram_at = functools.partial(packed_at, gram)

    def gram_of(v, chunk):
        if not chunk:
            for i in range(dim // BLK):
                zi = hbuf[view[v], span(i, dim)]
                sq = dot(zi, zi, TN)
                for row, lane, r, c, size, _ in PIECES[3 * i:3 * i + 3]:
                    gram_at(v, row, lane, size)[...] = sq[r - i * BLK:r - i * BLK + size, c - i * BLK:c - i * BLK + size]
        lo, hi = SPANS[chunk]
        for b, (i, j) in enumerate(OFF_PAIRS):
            row = TRI_ROWS + b * BLK
            if lo <= row < hi:
                gram_at(v, row, 0, BLK)[...] = dot(hbuf[view[v], span(i, dim)], hbuf[view[v], span(j, dim)], TN)
        reds[v][chunk].begin()

    reds = []
    for v in (0, 1):
        pair = []
        for ch, (lo, hi) in enumerate(SPANS):
            n, bd = hi - lo, band(v, ch)
            r1 = [net.at[pl.ds(k * n // 8, n // 8), bd] for k in (0, 1)]
            r2 = [net.at[pl.ds(n // 4 + k * n // 16, n // 16), bd] for k in (0, 1)]
            pair.append(GramReduce(place, gram.at[pl.ds(0, n), bd], ghat.at[v, pl.ds(lo, n)], part.at[pl.ds(0, n // 2), bd], r1, r2,
                                   rd_ss.at[2 * v + ch], rd_rs.at[2 * v + ch]))
        reds.append(pair)
    (a0, a1), (b0, b1) = reds

    def store_outer(mus):
        for v in (0, 1):
            for row, lane, r, c, size, _ in PIECES:
                col = jnp.transpose(jnp.broadcast_to(mus[v][:, r:r + size], (size, size)))
                packed_at(outer, v, row, lane, size)[...] = (all_rows * col) * mus[v][:, c:c + size]

    def finish(v, ch):
        def fin(row, acc):
            leaf = acc.shape[0]
            prow = SPANS[ch][0] + row + lax.broadcasted_iota(jnp.int32, acc.shape, 0)
            lane = lax.broadcasted_iota(jnp.int32, acc.shape, 1)
            quad = (prow < TRI_ROWS) & ((prow >= DIAG_ROWS) | (lane < QUAD))
            eye = quad & (lax.rem(prow, QUAD) == lax.rem(lane, QUAD))
            cov = (acc - outer[pl.ds(row, leaf), band(v, ch)]) / (all_rows - 1)
            std = jnp.sqrt(cov + STD_EPS)
            hinge = jnp.where(eye, jnp.maximum(1.0 - std, 0.0), 0.0)
            off = jnp.where(eye, 0.0, cov * cov) * jnp.where(quad, 1.0, 2.0)
            term = col_sum(hinge + 2.0 * off)
            ls_src[0] = ls_src[0] + term[:, :LANES] + term[:, LANES:]
            on = jnp.where(std < 1.0, 1.0, 0.0)
            return jnp.where(eye, -on / (2.0 * std), 4.0 * cov).astype(BF16)
        return fin

    def expand(v):
        for row, lane, r, c, size, mirrored in PIECES:
            blk = ghat[v, row:row + size, lane:lane + size]
            w1b[v * dim + r:v * dim + r + size, c:c + size] = blk
            if mirrored:
                w1b[v * dim + c:v * dim + c + size, r:r + size] = jnp.transpose(blk)

    def grad_z(v, mu, between):
        hi = mu.astype(BF16)
        mid = (mu - hi.astype(F32)).astype(BF16)
        low = (mu - hi.astype(F32) - mid.astype(F32)).astype(BF16)
        parts = jnp.concatenate([hi, mid, low, jnp.zeros((13, dim), BF16)], axis=0)
        g = w1b.at[pl.ds(v * dim, dim)]
        mean_part = col_sum(dot(parts, g[...]))
        sign = -1.0 if v else 1.0

        for part in range(rows // ROWS):
            sub = pl.ds(part * ROWS, ROWS)
            za, zo, out = zb[0].at[sub], zb[1].at[sub], dzb.at[pl.ds(v * rows + part * ROWS, ROWS)]

            def use(rws, row_part):
                diff = za[rws, :].astype(F32) - zo[rws, :].astype(F32)
                dz = (2.0 / (all_rows - 1)) * (row_part - mean_part) + (sign * 4.0 / all_rows) * diff
                out[rws, :] = dz.astype(BF16)
                return ()

            by_rows(zb[v].at[sub], g, use)
            if between:
                between.pop(0)()

    chunks = Chunks(place, part, net, grads, rd_ss, rd_rs)

    def load_h(t):
        row, size = chunk_of(t)
        slot = lax.rem(t, 2)
        return [pltpu.make_async_copy(h.at[:, lanes(row - 2 * dim, size)], x2.at[view[v], lanes(slot * CHUNK, size)], h_sem.at[slot, v])
                for v, h in enumerate(h_all)]

    def weight_grad(t, lhs, rhs):
        dst = chunks.part_of(t)

        def half(j):
            cols = tile(j, ROWS)
            dst[:, cols] = dot(lhs[...], rhs[:, cols], TN)

        loop(dim // ROWS, half)
        chunks.reduce(t).begin()

    def grad_act(slot, v, layer, src, w):
        gain, bias = affine[layer]
        n_ref, dst = nb.at[view[v]], dxb.at[view[v]]

        def use(rws, dx):
            n = n_ref[rws, :]
            da = jnp.where(gain[...] * n + bias[...] > 0.0, dx, 0.0)
            dst[rws, :] = da
            return da, da * n

        st_src[slot, ROW0, :], st_src[slot, ROW1, :] = by_rows(src.at[view[v]], w, use, 2, NT)
        stats.send(slot)

    def grad_pre(slot, v, layer, dst):
        sums = stats.total(slot)
        for row, o in ((ROW1, 2 * layer), (ROW0, 2 * layer + 1)):
            bn_o[one(o), :] = bn_o[one(o), :] + sums[row] if v else sums[row]
        mean_d = sums[ROW0] / all_rows
        mean_dn = sums[ROW1] / all_rows
        scale = invs[one(2 * layer + v), :] * affine[layer][0][...]

        def body(i):
            rws = tile(i, STRIP, v * rows)
            dst[rws, :] = (scale * (dxb[rws, :] - mean_d - nb[rws, :] * mean_dn)).astype(BF16)

        loop(rows // STRIP, body)

    loads['w1'].wait()
    linear(0, u1.at[view[0]], hbuf.at[view[0]], w1b)
    loads['hb'].wait()
    linear(1, u1.at[view[1]], hbuf.at[view[1]], w1b)
    for name in list(loads):
        if name[0] not in 'h1' and name != 'w1':
            loads[name].wait()
    for v in (0, 1):
        norm_relu(v, v, 0, u1, x1)
        spill[v].start()
        linear(2 + v, nb.at[view[v]], x1.at[view[v]], w2b)
    zs_src[0] = jnp.zeros(zs_src.shape[1:], F32)
    ls_src[0] = jnp.zeros((1, LANES), F32)
    norm_relu(2, 0, 1, nb, x2)
    project(0)
    gram_of(0, 0)
    gram_of(0, 1)
    norm_relu(3, 1, 1, nb, x2)
    a0.step_1()
    a1.step_1()
    project(1)
    stats.drain()
    zstats.send(0)
    gram_of(1, 0)
    gram_of(1, 1)
    a0.step_2()
    b0.step_1()
    b1.step_1()
    a1.step_2()
    ztot = zstats.total(0)
    mus = [ztot[one(v)] / all_rows for v in (0, 1)]
    sq_sum = jnp.sum(ztot[one(2)])
    for cp in spill:
        cp.wait()
    store_outer(mus)
    a0.step_3(finish(0, 0))
    a1.step_3(finish(0, 1))
    b0.step_2()
    a0.step_4()
    b1.step_2()
    a1.step_4()
    b0.step_3(finish(1, 0))
    b1.step_3(finish(1, 1))
    lstats.send(0)
    b0.step_4()
    a0.step_5()
    b1.step_4()
    a1.step_5()
    a0.step_6()
    a1.step_6()
    expand(0)
    grad_z(0, mus[0], [b0.step_5])
    lead = lanes(0, chunk_of(0)[1])
    chunks.part_of(0)[...] = dot(x2[view[0], lead], dzb[view[0], :], TN)
    b1.step_5()
    b0.step_6()
    b1.step_6()
    expand(1)
    grad_z(1, mus[1], [])
    zstats.drain()
    for red in (a0, a1, b0, b1):
        red.drain_part()
        red.drain_full()

    dub, du1 = w1b, hbuf.at[:, zcol]
    first_two = next(t for t in range(COUNT) if chunk_of(t)[0] >= dim)
    first_one = next(t for t in range(COUNT) if chunk_of(t)[0] >= 2 * dim)
    extra = {
        first_two - 2: lambda: grad_act(4, 0, 1, dzb, w3b),
        first_two - 1: lambda: grad_act(5, 1, 1, dzb, w3b),
        first_two: lambda: (load_n1[0].wait(), grad_act(6, 0, 0, dub, w2b)),
        first_two + 1: lambda: (load_n1[1].wait(), grad_act(7, 1, 0, dub, w2b)),
        first_two + 2: lambda: grad_pre(6, 0, 0, du1),
        first_two + 3: lambda: (grad_pre(7, 1, 0, du1), [cp.start() for cp in load_h(first_one)]),
    }

    def weight_tick(t):
        for cp in load_h(t):
            cp.wait()
        if not isinstance(t, int) or t + 1 < COUNT:
            for cp in load_h(t + 1):
                cp.start()
        weight_grad(t, x2.at[:, lanes(lax.rem(t, 2) * CHUNK, chunk_of(t)[1])], du1)

    for t in range(first_one):
        early = t < PART_SLOTS
        chunks.steps(t, 1, t - 1 if early else LAST_STEP)
        if t == first_two:
            for v in (0, 1):
                grad_pre(4 + v, v, 1, dub)
                load_n1[v].start()
        row, size = chunk_of(t)
        if not t:
            chunks.part_of(t)[...] = chunks.part_of(t)[...] + dot(x2[view[1], lead], dzb[view[1], :], TN)
            chunks.reduce(t).begin()
        elif t < first_two:
            weight_grad(t, x2.at[:, lanes(row, size)], dzb)
        else:
            weight_grad(t, x1.at[:, lanes(row - dim, size)], dub)
        if early:
            chunks.steps(t, max(t, 1))
        if t in extra:
            extra[t]()

    def tick(t):
        chunks.steps(t)
        weight_tick(t)

    last_even = LEAD + EVEN - 1
    loop(last_even - first_one, lambda i: tick(first_one + i))
    for t in range(last_even, COUNT + LAST_STEP):
        chunks.steps(t)
        if t < COUNT:
            weight_tick(t)
    loss_o[...] = jnp.broadcast_to(jnp.sum(lstats.total(0)) + 2.0 * sq_sum / all_rows, loss_o.shape)
    stats.drain()
    lstats.drain()


def train_step(n_dev, h_a, h_b, w1, w2, w3, *affine):
    rows, feat = h_a.shape
    dim = w2.shape[0]
    total = 2 * dim + feat
    any_spec = pl.BlockSpec(memory_space=pl.ANY)
    vm = pl.BlockSpec(memory_space=pltpu.VMEM)
    dma = pltpu.SemaphoreType.DMA
    wide = (2 * rows, dim)
    moments = (2, dim)
    return pl.pallas_call(
        functools.partial(step_kernel, rows * n_dev),
        name='train_step',
        out_shape=[pltpu.VMEM((total, dim), F32), pltpu.VMEM((4, dim), F32), pltpu.VMEM((1, LANES), F32), jax.ShapeDtypeStruct(wide, F32)],
        in_specs=[any_spec] * 9,
        out_specs=[vm] * 3 + [any_spec],
        scratch_shapes=[
            pltpu.VMEM((4, 1, dim), F32), pltpu.VMEM((2 * rows, feat), BF16), pltpu.VMEM((feat, dim), BF16), pltpu.VMEM((dim, dim), BF16), pltpu.VMEM((dim, dim), BF16),
            pltpu.VMEM(wide, BF16), pltpu.VMEM(wide, BF16), pltpu.VMEM(wide, F32), pltpu.VMEM((2, PACKED, BLK), BF16),
            pltpu.VMEM((PART_SLOTS * CHUNK, dim), F32), pltpu.VMEM((CORE_SLOTS * CHUNK // 2 + LINK_SLOTS * CHUNK * 3 // 8, dim), F32),
            pltpu.VMEM((4, dim), F32),
            pltpu.VMEM((8,) + moments, F32), pltpu.VMEM((8, NDEV) + moments, F32),
            pltpu.VMEM((1, 4, dim), F32), pltpu.VMEM((1, NDEV, 4, dim), F32),
            pltpu.VMEM((1, 1, LANES), F32), pltpu.VMEM((1, NDEV, 1, LANES), F32),
            dma((8 + rows // ROWS,)), dma((2,)), dma((2, 2)), dma((SETS, NDEV)), dma((SETS, NDEV)), dma((1, NDEV)), dma((1, NDEV)),
            dma((SETS, 10)), dma((SETS, 10))],
        compiler_params=pltpu.CompilerParams(collective_id=0, has_side_effects=True, vmem_limit_bytes=VMEM_BYTES - total * dim * 4 - SPARE),
    )(h_a, h_b, w1, w2, w3, *affine)


def emit_kernel(rows, grads, bn, loss, *refs):
    outs, sem = refs[:-1], refs[-1]
    srcs = [grads.at[pl.ds(lo, hi - lo)] for lo, hi in rows] + [bn.at[one(i)] for i in range(4)] + [loss]
    copies = [pltpu.make_async_copy(src, dst, sem.at[i]) for i, (src, dst) in enumerate(zip(srcs, outs))]
    for cp in copies:
        cp.start()
    for cp in copies:
        cp.wait()


def emit(grads, bn, loss, dim):
    total = grads.shape[0]
    rows = ((2 * dim, total), (dim, 2 * dim), (0, dim))
    any_spec = pl.BlockSpec(memory_space=pl.ANY)
    vm = pl.BlockSpec(memory_space=pltpu.VMEM)
    vec = jax.ShapeDtypeStruct((1, dim), F32)
    return pl.pallas_call(
        functools.partial(emit_kernel, rows),
        name='emit',
        out_shape=[jax.ShapeDtypeStruct((hi - lo, dim), F32) for lo, hi in rows] + [vec] * 4 + [jax.ShapeDtypeStruct((1, LANES), F32)],
        in_specs=[vm, vm, vm],
        out_specs=[any_spec] * 8,
        scratch_shapes=[pltpu.SemaphoreType.DMA((8,))],
        compiler_params=pltpu.CompilerParams(vmem_limit_bytes=VMEM_BYTES // 16),
    )(*(pltpu.with_memory_space_constraint(v, pltpu.VMEM) for v in (grads, bn, loss)))


def solution(mesh):
    n_dev = mesh.shape['data']

    def local_step(h_a, h_b, w_one, w_two, w_three, gain_one, bias_one, gain_two, bias_two):
        affine = [v.reshape(1, -1) for v in (gain_one, bias_one, gain_two, bias_two)]
        grads, bn, loss, _ = train_step(n_dev, h_a, h_b, w_one, w_two, w_three, *affine)
        d_one, d_two, d_three, *small, loss = emit(grads, bn, loss, w_two.shape[0])
        return (loss[0, 0], d_one, d_two, d_three) + tuple(v.reshape(-1) for v in small)

    row = P('data', None)
    return jax.shard_map(local_step, mesh=mesh, in_specs=(row, row) + (P(),) * 7, out_specs=(P(),) * 8, check_vma=False)
```

```python
import functools

import jax
import jax.numpy as jnp
from jax import lax
from jax.experimental import pallas as pl
from jax.experimental.pallas import tpu as pltpu
from jax.sharding import PartitionSpec as P

BN_EPS = 1e-5
STD_EPS = 1e-4
F32 = jnp.float32
BF16 = jnp.bfloat16
MESH = pl.DeviceIdType.MESH
NDEV = 8
BLK = 256
STRIP = 64
SETS = 4
SPARE = 524288
ROWS = 512
VMEM_BYTES = 67043328
LANES = 128
QUAD = 128
DIAG_ROWS = 4 * QUAD
TRI_ROWS = 6 * QUAD
OFF_PAIRS = [(0, 1), (0, 2), (0, 3), (1, 2), (1, 3), (2, 3)]
PIECES = []
for _i in range(4):
    _b = _i * BLK
    PIECES += [(_i * QUAD, 0, _b, _b, QUAD, False), (_i * QUAD, QUAD, _b, _b + QUAD, QUAD, True),
               (DIAG_ROWS + _i // 2 * QUAD, _i % 2 * QUAD, _b + QUAD, _b + QUAD, QUAD, False)]
PIECES += [(TRI_ROWS + _b * BLK, 0, _i * BLK, _j * BLK, BLK, True) for _b, (_i, _j) in enumerate(OFF_PAIRS)]
PACKED = TRI_ROWS + len(OFF_PAIRS) * BLK
SPLIT = TRI_ROWS + 2 * BLK
SPANS = ((0, SPLIT), (SPLIT, PACKED))
ROW0, ROW1 = slice(0, 1), slice(1, 2)
TN = (((0,), (0,)), ((), ()))
NT = (((1,), (1,)), ((), ()))


def dot(a, b, dims=(((1,), (0,)), ((), ()))):
    return lax.dot_general(a, b, dims, preferred_element_type=F32)


def col_sum(v):
    return jnp.sum(v, axis=0, keepdims=True)


def one(i):
    return slice(i, i + 1)


def tile(j, size=BLK, base=0):
    return pl.ds(pl.multiple_of(base + j * size, size), size)


def span(i, base=0):
    return slice(base + i * BLK, base + i * BLK + BLK)


def loop(count, body):
    def step(i, carry):
        body(i)
        return carry

    lax.fori_loop(0, count, step, 0)


class Place:
    def __init__(self):
        me = lax.axis_index('data')
        self.me = me
        self.c = lax.rem(me, 2)
        self.x = lax.rem(me // 2, 2)
        self.y = me // 4

    def flip(self, dy, dx, dc):
        y = 1 - self.y if dy else self.y
        x = 1 - self.x if dx else self.x
        c = 1 - self.c if dc else self.c
        return y * 4 + x * 2 + c

    def peer(self, o):
        return self.flip(o & 4, o & 2, o & 1)


def greet(place):
    barrier = pltpu.get_barrier_semaphore()
    for o in range(1, NDEV):
        pl.semaphore_signal(barrier, inc=1, device_id=(place.peer(o),), device_id_type=MESH)


def meet():
    pl.semaphore_wait(pltpu.get_barrier_semaphore(), NDEV - 1)


class StatExchange:
    def __init__(self, place, src, rcv, ssem, rsem):
        self.place, self.src, self.rcv, self.ssem, self.rsem = place, src, rcv, ssem, rsem
        self.sent = []

    def copies(self, slot):
        place = self.place
        return [pltpu.make_async_remote_copy(
            src_ref=self.src.at[slot], dst_ref=self.rcv.at[slot, place.me],
            send_sem=self.ssem.at[slot % SETS, o], recv_sem=self.rsem.at[slot % SETS, o],
            device_id=(place.peer(o),), device_id_type=MESH) for o in range(1, NDEV)]

    def send(self, slot):
        self.rcv[slot, self.place.me] = self.src[slot]
        for cp in self.copies(slot):
            cp.start()
        self.sent.append(slot)

    def total(self, slot):
        for cp in self.copies(slot):
            cp.wait_recv()
        acc = self.rcv[slot, 0]
        for d in range(1, NDEV):
            acc = acc + self.rcv[slot, d]
        return acc

    def drain(self):
        for slot in self.sent:
            for cp in self.copies(slot):
                cp.wait_send()
        self.sent = []


class Reduce:
    def __init__(self, place, part, full, rc, r1, r2, ssem, rsem):
        self.place, self.part, self.full = place, part, full
        self.ssem, self.rsem = ssem, rsem
        self.rows = part.shape[0]
        self.rc, self.r1, self.r2 = rc, r1, r2
        place_pq = [(place.x, place.y), (place.y, place.x)]
        rows, c = self.rows, place.c
        al = rows // 16
        self.leaf_rows = al
        mo = lambda v: pl.multiple_of(v, al)
        self.half_mine = mo(c * (rows // 2))
        self.half_other = mo((1 - c) * (rows // 2))
        self.o1_mine, self.o1_other, self.o2_mine, self.o2_other = [], [], [], []
        for k, (p, q) in enumerate(place_pq):
            base = c * (rows // 2) + k * (rows // 4)
            self.o1_mine.append(mo(base + p * (rows // 8)))
            self.o1_other.append(mo(base + (1 - p) * (rows // 8)))
            self.o2_mine.append(mo(base + p * (rows // 8) + q * (rows // 16)))
            self.o2_other.append(mo(base + p * (rows // 8) + (1 - q) * (rows // 16)))
        self.dev_c = place.flip(0, 0, 1)
        self.dev_1 = [place.flip(0, 1, 0), place.flip(1, 0, 0)]
        self.dev_2 = [place.flip(1, 0, 0), place.flip(0, 1, 0)]

    def _cp(self, idx, src, dst, dev):
        return pltpu.make_async_remote_copy(src_ref=src, dst_ref=dst, send_sem=self.ssem.at[idx], recv_sem=self.rsem.at[idx],
                                            device_id=(dev,), device_id_type=MESH)

    def cp_c(self):
        return [self._cp(0, self.part.at[pl.ds(self.half_other, self.rows // 2)], self.rc, self.dev_c)]

    def cp_1(self):
        return [self._cp(1 + k, self.part.at[pl.ds(self.o1_other[k], self.rows // 8)], self.r1[k], self.dev_1[k]) for k in (0, 1)]

    def cp_2(self):
        return [self._cp(3 + k, self.part.at[pl.ds(self.o2_other[k], self.rows // 16)], self.r2[k], self.dev_2[k]) for k in (0, 1)]

    def cp_g2(self):
        return [self._cp(5 + k, self.full.at[pl.ds(self.o2_mine[k], self.rows // 16)],
                         self.full.at[pl.ds(self.o2_mine[k], self.rows // 16)], self.dev_2[k]) for k in (0, 1)]

    def cp_g1(self):
        return [self._cp(7 + k, self.full.at[pl.ds(self.o1_mine[k], self.rows // 8)],
                         self.full.at[pl.ds(self.o1_mine[k], self.rows // 8)], self.dev_1[k]) for k in (0, 1)]

    def cp_gc(self):
        half = pl.ds(self.half_mine, self.rows // 2)
        return [self._cp(9, self.full.at[half], self.full.at[half], self.dev_c)]

    @staticmethod
    def start(cps):
        for cp in cps:
            cp.start()

    def begin(self):
        self.start(self.cp_c())

    def step_1(self):
        self.cp_c()[0].wait_recv()
        mine = pl.ds(self.half_mine, self.rows // 2)
        self.part[mine] = self.part[mine] + self.rc[...]
        self.start(self.cp_1())

    def step_2(self):
        for k, (cp, nxt) in enumerate(zip(self.cp_1(), self.cp_2())):
            cp.wait_recv()
            mine = pl.ds(self.o1_mine[k], self.rows // 8)
            self.part[mine] = self.part[mine] + self.r1[k][...]
            nxt.start()

    def step_3(self, finish):
        for k, (cp, nxt) in enumerate(zip(self.cp_2(), self.cp_g2())):
            cp.wait_recv()
            mine = pl.ds(self.o2_mine[k], self.rows // 16)
            self.full[mine] = finish(self.o2_mine[k], self.part[mine] + self.r2[k][...])
            nxt.start()

    def step_4(self):
        for cp in self.cp_g2():
            cp.wait_recv()
        self.start(self.cp_g1())

    def step_5(self):
        for cp in self.cp_g1():
            cp.wait_recv()
        self.start(self.cp_gc())

    def step_6(self):
        self.cp_gc()[0].wait_recv()

    def drain_part(self):
        for cp in self.cp_c() + self.cp_1() + self.cp_2():
            cp.wait_send()

    def drain_full(self):
        for cp in self.cp_g2() + self.cp_g1() + self.cp_gc():
            cp.wait_send()


def by_rows(lhs, rhs, use, sums=0, dims=(((1,), (0,)), ((), ()))):
    def step(i, carry):
        rws = tile(i, ROWS)
        terms = use(rws, dot(lhs[rws, :], rhs[...], dims))
        return tuple(c + col_sum(t) for c, t in zip(carry, terms))

    width = rhs.shape[1 - dims[0][1][0]]
    return lax.fori_loop(0, lhs.shape[0] // ROWS, step, (jnp.zeros((1, width), F32),) * sums)


CHUNK, SMALL = 256, 128
LEAD, EVEN, TAIL = 0, 16, 0
COUNT = LEAD + EVEN + TAIL
PART_SLOTS, CORE_SLOTS, LINK_SLOTS = 3, 3, 4
LAST_STEP = 6


def chunk_of(t):
    if not isinstance(t, int) or LEAD <= t < LEAD + EVEN:
        return (t - LEAD) * CHUNK + LEAD * SMALL, CHUNK
    if t < LEAD:
        return t * SMALL, SMALL
    return EVEN * CHUNK + (t - EVEN) * SMALL, SMALL


class Chunks:
    def __init__(self, place, part, net, out, ssem, rsem):
        self.place, self.part, self.net, self.out = place, part, net, out
        self.ssem, self.rsem = ssem, rsem

    def reduce(self, t):
        row, size = chunk_of(t)
        link = lax.rem(t, LINK_SLOTS)

        def landing(base, slot, room, used):
            return self.net.at[pl.ds(pl.multiple_of(base + slot * room, 8), used)]

        one_base = CORE_SLOTS * CHUNK // 2
        two_base = one_base + LINK_SLOTS * CHUNK // 4
        return Reduce(self.place, self.part_of(t), self.out.at[pl.ds(pl.multiple_of(row, SMALL), size)],
                      landing(0, lax.rem(t, CORE_SLOTS), CHUNK // 2, size // 2),
                      [landing(one_base, 2 * link + k, CHUNK // 8, size // 8) for k in (0, 1)],
                      [landing(two_base, 2 * link + k, CHUNK // 16, size // 16) for k in (0, 1)], self.ssem.at[lax.rem(t, SETS)], self.rsem.at[lax.rem(t, SETS)])

    def part_of(self, t):
        return self.part.at[pl.ds(pl.multiple_of(lax.rem(t, PART_SLOTS) * CHUNK, CHUNK), chunk_of(t)[1])]

    def step(self, k, t):
        red = self.reduce(t)
        if k == 3:
            red.step_3(lambda row, acc: acc)
            red.drain_part()
        else:
            getattr(red, 'step_%d' % k)()
        if k == LAST_STEP:
            red.drain_full()

    def steps(self, t, first=1, last=LAST_STEP):
        for k in range(first, last + 1):
            if not isinstance(t, int) or 0 <= t - k < COUNT:
                self.step(k, t - k)


GramReduce = Reduce


def step_kernel(all_rows, h_a, h_b, w1, w2, w3, g1, b1, g2, b2,
                grads, bn_o, loss_o, n1_o,
                affine_b, hbuf, w1b, w2b, w3b, x1, x2, nb, ghat, part, net, invs,
                st_src, st_rcv, zs_src, zs_rcv, ls_src, ls_rcv,
                ld_sem, n_sem, h_sem, st_ss, st_rs, ls_ss, ls_rs, rd_ss, rd_rs):
    dim = w2b.shape[0]
    rows, feat = h_a.shape
    affine = ((affine_b.at[0], affine_b.at[1]), (affine_b.at[2], affine_b.at[3]))
    view = [slice(0, rows), slice(rows, 2 * rows)]
    low, high = slice(0, 2 * dim), slice(2 * dim, 2 * dim + feat)
    u1, dxb = grads.at[low], grads.at[high]
    place = Place()
    greet(place)
    h_all = (h_a, h_b)
    strip = lambda i: slice(i * ROWS, i * ROWS + ROWS)
    loads = {}
    for name, src, dst in (('w1', w1, w1b), *(('ha%d' % i, h_a.at[strip(i)], hbuf.at[strip(i)]) for i in range(rows // ROWS)), ('hb', h_b, hbuf.at[view[1]]), ('w2', w2, w2b), ('w3', w3, w3b),
                           *(('affine%d' % i, src, affine_b.at[i]) for i, src in enumerate((g1, b1, g2, b2)))):
        loads[name] = pltpu.make_async_copy(src, dst, ld_sem.at[len(loads)])
        loads[name].start()
    spill = [pltpu.make_async_copy(u1.at[view[v]], n1_o.at[view[v]], n_sem.at[v]) for v in (0, 1)]
    load_n1 = [pltpu.make_async_copy(n1_o.at[view[v]], nb.at[view[v]], n_sem.at[v]) for v in (0, 1)]

    def lanes(row, size):
        return pl.ds(pl.multiple_of(row, SMALL), size)

    stats = StatExchange(place, st_src, st_rcv, st_ss, st_rs)
    zstats = StatExchange(place, zs_src, zs_rcv, st_ss, st_rs)
    lstats = StatExchange(place, ls_src, ls_rcv, ls_ss, ls_rs)

    def linear(slot, dst, lhs, rhs):
        def use(rws, out):
            dst[rws, :] = out
            return out, out * out

        if slot:
            sums = by_rows(lhs, rhs, use, 2)
        else:
            sums = None
            for i in range(rows // ROWS):
                loads['ha%d' % i].wait()
                out = dot(lhs[strip(i), :], rhs[...])
                terms = [col_sum(t) for t in use(strip(i), out)]
                sums = [a + b for a, b in zip(sums, terms)] if i else terms
            meet()
        st_src[slot, ROW0, :], st_src[slot, ROW1, :] = sums
        stats.send(slot)

    def norm_relu(slot, v, layer, ubuf, xbuf):
        mom = stats.total(slot)
        mean = mom[ROW0] / all_rows
        var = mom[ROW1] / all_rows - mean * mean
        inv = lax.rsqrt(var + BN_EPS)
        invs[one(slot), :] = inv
        gain, bias = affine[layer]

        def body(i):
            rws = tile(i, STRIP, v * rows)
            n = (ubuf[rws, :] - mean) * inv
            ubuf[rws, :] = n
            xbuf[rws, :] = jnp.maximum(gain[...] * n + bias[...], 0.0).astype(BF16)

        loop(rows // STRIP, body)

    zcol = pl.ds(dim, dim)
    dzb = hbuf.at[:, pl.ds(0, dim)]
    zb = [hbuf.at[view[v], zcol] for v in (0, 1)]

    def project(v):
        def use(rws, out):
            z = out.astype(BF16)
            zb[v][rws, :] = z
            zf = z.astype(F32)
            if not v:
                return zf,
            diff = zb[0][rws, :].astype(F32) - zf
            return zf, diff * diff

        for o, term in enumerate(by_rows(x2.at[view[v]], w3b, use, 1 + v)):
            zs_src[0, one(v + o), :] = term

    outer, gram = grads.at[low], grads.at[high]

    def band(v, ch):
        return pl.ds((2 * v + ch) * BLK, BLK)

    def packed_at(ref, v, row, lane, size):
        ch = int(row >= SPLIT)
        return ref.at[pl.ds(row - SPANS[ch][0], size), pl.ds((2 * v + ch) * BLK + lane, size)]

    gram_at = functools.partial(packed_at, gram)

    def gram_of(v, chunk):
        if not chunk:
            for i in range(dim // BLK):
                zi = hbuf[view[v], span(i, dim)]
                sq = dot(zi, zi, TN)
                for row, lane, r, c, size, _ in PIECES[3 * i:3 * i + 3]:
                    gram_at(v, row, lane, size)[...] = sq[r - i * BLK:r - i * BLK + size, c - i * BLK:c - i * BLK + size]
        lo, hi = SPANS[chunk]
        for b, (i, j) in enumerate(OFF_PAIRS):
            row = TRI_ROWS + b * BLK
            if lo <= row < hi:
                gram_at(v, row, 0, BLK)[...] = dot(hbuf[view[v], span(i, dim)], hbuf[view[v], span(j, dim)], TN)
        reds[v][chunk].begin()

    reds = []
    for v in (0, 1):
        pair = []
        for ch, (lo, hi) in enumerate(SPANS):
            n, bd = hi - lo, band(v, ch)
            r1 = [net.at[pl.ds(k * n // 8, n // 8), bd] for k in (0, 1)]
            r2 = [net.at[pl.ds(n // 4 + k * n // 16, n // 16), bd] for k in (0, 1)]
            pair.append(GramReduce(place, gram.at[pl.ds(0, n), bd], ghat.at[v, pl.ds(lo, n)], part.at[pl.ds(0, n // 2), bd], r1, r2,
                                   rd_ss.at[2 * v + ch], rd_rs.at[2 * v + ch]))
        reds.append(pair)
    (a0, a1), (b0, b1) = reds

    def store_outer(mus):
        for v in (0, 1):
            for row, lane, r, c, size, _ in PIECES:
                col = jnp.transpose(jnp.broadcast_to(mus[v][:, r:r + size], (size, size)))
                packed_at(outer, v, row, lane, size)[...] = (all_rows * col) * mus[v][:, c:c + size]

    def finish(v, ch):
        def fin(row, acc):
            leaf = acc.shape[0]
            prow = SPANS[ch][0] + row + lax.broadcasted_iota(jnp.int32, acc.shape, 0)
            lane = lax.broadcasted_iota(jnp.int32, acc.shape, 1)
            quad = (prow < TRI_ROWS) & ((prow >= DIAG_ROWS) | (lane < QUAD))
            eye = quad & (lax.rem(prow, QUAD) == lax.rem(lane, QUAD))
            cov = (acc - outer[pl.ds(row, leaf), band(v, ch)]) / (all_rows - 1)
            std = jnp.sqrt(cov + STD_EPS)
            hinge = jnp.where(eye, jnp.maximum(1.0 - std, 0.0), 0.0)
            off = jnp.where(eye, 0.0, cov * cov) * jnp.where(quad, 1.0, 2.0)
            term = col_sum(hinge + 2.0 * off)
            ls_src[0] = ls_src[0] + term[:, :LANES] + term[:, LANES:]
            on = jnp.where(std < 1.0, 1.0, 0.0)
            return jnp.where(eye, -on / (2.0 * std), 4.0 * cov).astype(BF16)
        return fin

    def expand(v, ch):
        for row, lane, r, c, size, mirrored in PIECES:
            if int(row >= SPLIT) != ch:
                continue
            blk = ghat[v, row:row + size, lane:lane + size]
            w1b[v * dim + r:v * dim + r + size, c:c + size] = blk
            if mirrored:
                w1b[v * dim + c:v * dim + c + size, r:r + size] = jnp.transpose(blk)

    def grad_z(v, mu, between):
        hi = mu.astype(BF16)
        mid = (mu - hi.astype(F32)).astype(BF16)
        low = (mu - hi.astype(F32) - mid.astype(F32)).astype(BF16)
        parts = jnp.concatenate([hi, mid, low, jnp.zeros((13, dim), BF16)], axis=0)
        g = w1b.at[pl.ds(v * dim, dim)]
        mean_part = col_sum(dot(parts, g[...]))
        sign = -1.0 if v else 1.0

        for part in range(rows // ROWS):
            sub = pl.ds(part * ROWS, ROWS)
            za, zo, out = zb[0].at[sub], zb[1].at[sub], dzb.at[pl.ds(v * rows + part * ROWS, ROWS)]

            def use(rws, row_part):
                diff = za[rws, :].astype(F32) - zo[rws, :].astype(F32)
                dz = (2.0 / (all_rows - 1)) * (row_part - mean_part) + (sign * 4.0 / all_rows) * diff
                out[rws, :] = dz.astype(BF16)
                return ()

            by_rows(zb[v].at[sub], g, use)
            if between:
                between.pop(0)()

    chunks = Chunks(place, part, net, grads, rd_ss, rd_rs)

    def load_h(t):
        row, size = chunk_of(t)
        slot = lax.rem(t, 2)
        return [pltpu.make_async_copy(h.at[:, lanes(row - 2 * dim, size)], x2.at[view[v], lanes(slot * CHUNK, size)], h_sem.at[slot, v])
                for v, h in enumerate(h_all)]

    def weight_grad(t, lhs, rhs):
        dst = chunks.part_of(t)

        def half(j):
            cols = tile(j, ROWS)
            dst[:, cols] = dot(lhs[...], rhs[:, cols], TN)

        loop(dim // ROWS, half)
        chunks.reduce(t).begin()

    def grad_act(slot, v, layer, src, w):
        gain, bias = affine[layer]
        n_ref, dst = nb.at[view[v]], dxb.at[view[v]]

        def use(rws, dx):
            n = n_ref[rws, :]
            da = jnp.where(gain[...] * n + bias[...] > 0.0, dx, 0.0)
            dst[rws, :] = da
            return da, da * n

        st_src[slot, ROW0, :], st_src[slot, ROW1, :] = by_rows(src.at[view[v]], w, use, 2, NT)
        stats.send(slot)

    def grad_pre(slot, v, layer, dst):
        sums = stats.total(slot)
        for row, o in ((ROW1, 2 * layer), (ROW0, 2 * layer + 1)):
            bn_o[one(o), :] = bn_o[one(o), :] + sums[row] if v else sums[row]
        mean_d = sums[ROW0] / all_rows
        mean_dn = sums[ROW1] / all_rows
        scale = invs[one(2 * layer + v), :] * affine[layer][0][...]

        def body(i):
            rws = tile(i, STRIP, v * rows)
            dst[rws, :] = (scale * (dxb[rws, :] - mean_d - nb[rws, :] * mean_dn)).astype(BF16)

        loop(rows // STRIP, body)

    loads['w1'].wait()
    linear(0, u1.at[view[0]], hbuf.at[view[0]], w1b)
    loads['hb'].wait()
    linear(1, u1.at[view[1]], hbuf.at[view[1]], w1b)
    for name in list(loads):
        if name[0] not in 'h1' and name != 'w1':
            loads[name].wait()
    for v in (0, 1):
        norm_relu(v, v, 0, u1, x1)
        spill[v].start()
        linear(2 + v, nb.at[view[v]], x1.at[view[v]], w2b)
    zs_src[0] = jnp.zeros(zs_src.shape[1:], F32)
    ls_src[0] = jnp.zeros((1, LANES), F32)
    norm_relu(2, 0, 1, nb, x2)
    project(0)
    gram_of(0, 0)
    gram_of(0, 1)
    norm_relu(3, 1, 1, nb, x2)
    a0.step_1()
    a1.step_1()
    project(1)
    stats.drain()
    zstats.send(0)
    gram_of(1, 0)
    gram_of(1, 1)
    a0.step_2()
    b0.step_1()
    b1.step_1()
    a1.step_2()
    ztot = zstats.total(0)
    mus = [ztot[one(v)] / all_rows for v in (0, 1)]
    sq_sum = jnp.sum(ztot[one(2)])
    for cp in spill:
        cp.wait()
    store_outer(mus)
    a0.step_3(finish(0, 0))
    a1.step_3(finish(0, 1))
    b0.step_2()
    a0.step_4()
    b1.step_2()
    a1.step_4()
    b0.step_3(finish(1, 0))
    b1.step_3(finish(1, 1))
    lstats.send(0)
    b0.step_4()
    a0.step_5()
    b1.step_4()
    a1.step_5()
    a0.step_6()
    expand(0, 0)
    a1.step_6()
    expand(0, 1)
    grad_z(0, mus[0], [b0.step_5])
    lead = lanes(0, chunk_of(0)[1])
    chunks.part_of(0)[...] = dot(x2[view[0], lead], dzb[view[0], :], TN)
    b1.step_5()
    b0.step_6()
    expand(1, 0)
    b1.step_6()
    expand(1, 1)
    grad_z(1, mus[1], [])
    zstats.drain()
    for red in (a0, a1, b0, b1):
        red.drain_part()
        red.drain_full()

    dub, du1 = w1b, hbuf.at[:, zcol]
    first_two = next(t for t in range(COUNT) if chunk_of(t)[0] >= dim)
    first_one = next(t for t in range(COUNT) if chunk_of(t)[0] >= 2 * dim)
    extra = {
        first_two - 2: lambda: grad_act(4, 0, 1, dzb, w3b),
        first_two - 1: lambda: grad_act(5, 1, 1, dzb, w3b),
        first_two: lambda: (load_n1[0].wait(), grad_act(6, 0, 0, dub, w2b)),
        first_two + 1: lambda: (load_n1[1].wait(), grad_act(7, 1, 0, dub, w2b)),
        first_two + 2: lambda: grad_pre(6, 0, 0, du1),
        first_two + 3: lambda: (grad_pre(7, 1, 0, du1), [cp.start() for cp in load_h(first_one)]),
    }

    def weight_tick(t):
        for cp in load_h(t):
            cp.wait()
        if not isinstance(t, int) or t + 1 < COUNT:
            for cp in load_h(t + 1):
                cp.start()
        weight_grad(t, x2.at[:, lanes(lax.rem(t, 2) * CHUNK, chunk_of(t)[1])], du1)

    for t in range(first_one):
        early = t < PART_SLOTS
        chunks.steps(t, 1, t - 1 if early else LAST_STEP)
        if t == first_two:
            for v in (0, 1):
                grad_pre(4 + v, v, 1, dub)
                load_n1[v].start()
        row, size = chunk_of(t)
        if not t:
            chunks.part_of(t)[...] = chunks.part_of(t)[...] + dot(x2[view[1], lead], dzb[view[1], :], TN)
            chunks.reduce(t).begin()
        elif t < first_two:
            weight_grad(t, x2.at[:, lanes(row, size)], dzb)
        else:
            weight_grad(t, x1.at[:, lanes(row - dim, size)], dub)
        if early:
            chunks.steps(t, max(t, 1))
        if t in extra:
            extra[t]()

    def tick(t):
        chunks.steps(t)
        weight_tick(t)

    loss_o[...] = jnp.broadcast_to(jnp.sum(lstats.total(0)) + 2.0 * sq_sum / all_rows, loss_o.shape)
    stats.drain()
    lstats.drain()
    last_even = LEAD + EVEN - 1
    loop(last_even - first_one, lambda i: tick(first_one + i))
    for t in range(last_even, COUNT + LAST_STEP):
        chunks.steps(t)
        if t < COUNT:
            weight_tick(t)


def train_step(n_dev, h_a, h_b, w1, w2, w3, *affine):
    rows, feat = h_a.shape
    dim = w2.shape[0]
    total = 2 * dim + feat
    any_spec = pl.BlockSpec(memory_space=pl.ANY)
    vm = pl.BlockSpec(memory_space=pltpu.VMEM)
    dma = pltpu.SemaphoreType.DMA
    wide = (2 * rows, dim)
    moments = (2, dim)
    return pl.pallas_call(
        functools.partial(step_kernel, rows * n_dev),
        name='train_step',
        out_shape=[pltpu.VMEM((total, dim), F32), pltpu.VMEM((4, dim), F32), pltpu.VMEM((1, LANES), F32), jax.ShapeDtypeStruct(wide, F32)],
        in_specs=[any_spec] * 9,
        out_specs=[vm] * 3 + [any_spec],
        scratch_shapes=[
            pltpu.VMEM((4, 1, dim), F32), pltpu.VMEM((2 * rows, feat), BF16), pltpu.VMEM((feat, dim), BF16), pltpu.VMEM((dim, dim), BF16), pltpu.VMEM((dim, dim), BF16),
            pltpu.VMEM(wide, BF16), pltpu.VMEM(wide, BF16), pltpu.VMEM(wide, F32), pltpu.VMEM((2, PACKED, BLK), BF16),
            pltpu.VMEM((PART_SLOTS * CHUNK, dim), F32), pltpu.VMEM((CORE_SLOTS * CHUNK // 2 + LINK_SLOTS * CHUNK * 3 // 8, dim), F32),
            pltpu.VMEM((4, dim), F32),
            pltpu.VMEM((8,) + moments, F32), pltpu.VMEM((8, NDEV) + moments, F32),
            pltpu.VMEM((1, 4, dim), F32), pltpu.VMEM((1, NDEV, 4, dim), F32),
            pltpu.VMEM((1, 1, LANES), F32), pltpu.VMEM((1, NDEV, 1, LANES), F32),
            dma((8 + rows // ROWS,)), dma((2,)), dma((2, 2)), dma((SETS, NDEV)), dma((SETS, NDEV)), dma((1, NDEV)), dma((1, NDEV)),
            dma((SETS, 10)), dma((SETS, 10))],
        compiler_params=pltpu.CompilerParams(collective_id=0, has_side_effects=True, vmem_limit_bytes=VMEM_BYTES - total * dim * 4 - SPARE),
    )(h_a, h_b, w1, w2, w3, *affine)


def emit_kernel(rows, grads, bn, loss, *refs):
    outs, sem = refs[:-1], refs[-1]
    srcs = [grads.at[pl.ds(lo, hi - lo)] for lo, hi in rows] + [bn.at[one(i)] for i in range(4)] + [loss]
    copies = [pltpu.make_async_copy(src, dst, sem.at[i]) for i, (src, dst) in enumerate(zip(srcs, outs))]
    for cp in copies:
        cp.start()
    for cp in copies:
        cp.wait()


def emit(grads, bn, loss, dim):
    total = grads.shape[0]
    rows = ((2 * dim, total), (dim, 2 * dim), (0, dim))
    any_spec = pl.BlockSpec(memory_space=pl.ANY)
    vm = pl.BlockSpec(memory_space=pltpu.VMEM)
    vec = jax.ShapeDtypeStruct((1, dim), F32)
    return pl.pallas_call(
        functools.partial(emit_kernel, rows),
        name='emit',
        out_shape=[jax.ShapeDtypeStruct((hi - lo, dim), F32) for lo, hi in rows] + [vec] * 4 + [jax.ShapeDtypeStruct((1, LANES), F32)],
        in_specs=[vm, vm, vm],
        out_specs=[any_spec] * 8,
        scratch_shapes=[pltpu.SemaphoreType.DMA((8,))],
        compiler_params=pltpu.CompilerParams(vmem_limit_bytes=VMEM_BYTES // 16),
    )(*(pltpu.with_memory_space_constraint(v, pltpu.VMEM) for v in (grads, bn, loss)))


def solution(mesh):
    n_dev = mesh.shape['data']

    def local_step(h_a, h_b, w_one, w_two, w_three, gain_one, bias_one, gain_two, bias_two):
        affine = [v.reshape(1, -1) for v in (gain_one, bias_one, gain_two, bias_two)]
        grads, bn, loss, _ = train_step(n_dev, h_a, h_b, w_one, w_two, w_three, *affine)
        d_one, d_two, d_three, *small, loss = emit(grads, bn, loss, w_two.shape[0])
        return (loss[0, 0], d_one, d_two, d_three) + tuple(v.reshape(-1) for v in small)

    row = P('data', None)
    return jax.shard_map(local_step, mesh=mesh, in_specs=(row, row) + (P(),) * 7, out_specs=(P(),) * 8, check_vma=False)
```
